32 devices in a mesh: dp: 8 (over z, x), expert: 4 (over y, core).
Axes of the slice: x: 2, y: 2, z: 4, core: 2. Of those that a mesh axis runs over, the one named last changes fastest.
Arguments:
- images: bfloat16 [128, 197, 512], P(('dp', 'expert')), may hold values from -6 to 6
- adapter_ids: int32 [128], P(('dp', 'expert')), may hold values from 0 to 7
- expert_ids: int32 [128, 197, 2], P(('dp', 'expert')), may hold values from 0 to 15, all different within a row; in each aligned block of 788 rows (0 to 787, 788 to 1575, ..., all dimensions but the last counted through in order) at most 246 rows name the same one
- cotangent: bfloat16 [128, 197, 512], P(('dp', 'expert')), may hold values from -6 to 6
- ln_gain1: bfloat16 [512], replicated, may hold values from 0.099609375 to 1.8984375
- ln_gain2: bfloat16 [512], replicated, may hold values from 0.099609375 to 1.8984375
- qkv_weight: bfloat16 [512, 1536], replicated, may hold values from -0.25 to 0.25
- out_weight: bfloat16 [512, 512], replicated, may hold values from -1 to 1
- router_weight: bfloat16 [512, 16], replicated, may hold values from -0.1875 to 0.1875
- up_weight: bfloat16 [16, 512, 2048], P('expert'), may hold values from -0.25 to 0.25
- down_weight: bfloat16 [16, 2048, 512], P('expert'), may hold values from -0.125 to 0.125
- qkv_a: bfloat16 [8, 512, 16], replicated, may hold values from -0.25 to 0.25
- qkv_b: bfloat16 [8, 16, 1536], replicated, may hold values from -1 to 1
- out_a: bfloat16 [8, 512, 16], replicated, may hold values from -0.25 to 0.25
- out_b: bfloat16 [8, 16, 512], replicated, may hold values from -3 to 3
- router_a: bfloat16 [8, 512, 16], replicated, may hold values from -0.25 to 0.25
- router_b: bfloat16 [8, 16, 16], replicated, may hold values from -0.75 to 0.75
- up_a: bfloat16 [16, 8, 512, 16], P('expert'), may hold values from -0.25 to 0.25
- up_b: bfloat16 [16, 8, 16, 2048], P('expert'), may hold values from -1 to 1
- down_a: bfloat16 [16, 8, 2048, 16], P('expert'), may hold values from -0.125 to 0.125
- down_b: bfloat16 [16, 8, 16, 512], P('expert'), may hold values from -1 to 1
Outputs:
- block_out: bfloat16 [128, 197, 512], P(('dp', 'expert'))
- input_grad: float32 [128, 197, 512], P(('dp', 'expert'))
- grad_qkv_a: float32 [8, 512, 16], replicated
- grad_qkv_b: float32 [8, 16, 1536], replicated
- grad_out_a: float32 [8, 512, 16], replicated
- grad_out_b: float32 [8, 16, 512], replicated
- grad_router_a: float32 [8, 512, 16], replicated
- grad_router_b: float32 [8, 16, 16], replicated
- grad_up_a: float32 [16, 8, 512, 16], P('expert')
- grad_up_b: float32 [16, 8, 16, 2048], P('expert')
- grad_down_a: float32 [16, 8, 2048, 16], P('expert')
- grad_down_b: float32 [16, 8, 16, 512], P('expert')
The draws below stay inside these ranges and needn't reach their ends.
Inputs may be any that keep to these rules, and one draw needn't show every extreme that they name: `expert_ids`: each token names 2 different experts; among the tokens of one device no expert is named more than min(246, 788) times, and some expert is named exactly that often.
All inputs are finite; a program needn't handle non-finite values.
Results may differ from the reference program's by a relative error of at most 0.017.
Values may be sent and summed in bfloat16 or wider, within the bound.
A program may use at most 256 MiB of HBM per device.

```python
import math
import jax
import jax.numpy as jnp
import numpy as np
from jax import lax

D = 512
HEADS = 8
HD = 64
FF = 2048
TOPK = 2
SEQ = 197
NA = 8
R = 16
IMG_DEV = 4
E = 16
TOK_DEV = 788
IMAGES = 128
CAP = 123
N_DP = 8
N_EXPERT = 4


def set_ends(entries, stream_key, least, top_value):
    longest = entries.shape.index(max(entries.shape))
    spots = []
    for shift in (0, 1):
        where = [jax.random.randint(jax.random.fold_in(stream_key, axis), (), 0, length) for axis, length in enumerate(entries.shape)]
        where[longest] = (where[longest] + shift) % entries.shape[longest]
        spots.append(tuple(where))
    return entries.at[spots[0]].set(least).at[spots[1]].set(top_value)


def block_scale(stream_key, dims, shards, smallest, high):
    level, own = 1.0, jax.random.fold_in(stream_key, 6)
    for axis_at, parts in shards:
        heights = jnp.exp(jax.random.uniform(jax.random.fold_in(own, axis_at), (parts,), jnp.float32, smallest / len(shards), high / len(shards)))
        level = level * jnp.repeat(heights, dims[axis_at] // parts).reshape([-1 if axis == axis_at else 1 for axis in range(len(dims))])
    return level


def assign_block(own_key, own, number, rows, amount, top, limit, lean):
    order = jax.random.permutation(own_key, amount)
    packed, ordinary = portions_of(amount, rows * top, limit, lean, True), portions_of(amount, rows * top, limit, lean, False)
    places = jnp.arange(amount)

    def named(sizes, rotation):
        used = int((sizes > 0).sum())
        fixed = max(1, used // 4)
        shifted = fixed + (places - fixed + rotation * (used - fixed)) % max(1, amount - fixed)
        return jnp.zeros((amount,), jnp.int32).at[order[jnp.where(places < fixed, places, shifted)]].set(jnp.asarray(sizes, jnp.int32))

    sizes = jnp.where(number % 4 == 0, named(packed, number // 4), named(ordinary, number - number // 4 - 1))
    mixed = jax.random.permutation(jax.random.fold_in(own, 3), amount)
    source_of, sink = mixed[0:amount // 2 * 2:2], mixed[1:amount // 2 * 2:2]
    slack = jnp.minimum(sizes[source_of] - 1, limit - sizes[sink]) // 2
    slack = jnp.where((source_of == order[0]) | (sink == order[0]) | (sizes[sink] == 0), 0, jnp.maximum(slack, 0))
    shifted = jax.random.randint(jax.random.fold_in(own, 4), (amount // 2,), 0, 1 << 20) % (slack + 1)
    sizes = sizes.at[source_of].add(-shifted).at[sink].add(shifted)
    labels = jnp.searchsorted(jnp.cumsum(sizes), jnp.arange(rows * top), side="right").astype(jnp.int32)
    grid = labels.reshape(top, rows).T
    grid = grid[jax.random.permutation(jax.random.fold_in(own, 1), rows)]
    rotation = jax.random.randint(jax.random.fold_in(own, 2), (rows, 1), 0, top)
    return jnp.take_along_axis(grid, (jnp.arange(top)[None, :] + rotation) % top, axis=1)


def portions_of(amount, total, reach, lean, full):
    weights = [(1 << 20) // math.isqrt(standing ** lean) + 1 for standing in range(1, amount + 1)]
    largest = reach if full else min(reach, max(-(-total // amount), total * weights[0] // sum(weights)))
    least = 1 if total - largest >= amount - 1 else 0
    counts, spare = [largest] + [least] * (amount - 1), total - largest - least * (amount - 1)
    while spare > 0:
        movable = [i for i in range(1, amount) if counts[i] < largest] or [i for i in range(1, amount) if counts[i] < reach]
        mass, left = sum([weights[i] for i in movable]), spare
        for i in movable:
            extra = min(reach - counts[i], max(1, left * weights[i] // mass), spare)
            counts[i] = counts[i] + extra
            spare = spare - extra
    return np.array(counts)


def scatter_about(key, dims, width, reach, cuts=(), kind=jnp.bfloat16):
    entries = jax.random.normal(key, dims, jnp.float32) * width
    if len(cuts) > 0:
        entries = block_scale(key, dims, cuts, -0.22, 0.18) * entries
    return jnp.clip(entries, min=-reach, max=reach).astype(kind)


def setup_inputs(seed: int = 0) -> dict:
    key_list = jax.random.split(jax.random.key(seed), 22)
    images = scatter_about(key_list[0], (IMAGES, SEQ, D), 1.0, 6.0, ((0, 32),))
    adapter_ids = set_ends(jax.random.randint(key_list[1], (IMAGES,), 0, NA), jax.random.fold_in(key_list[1], 1), 0, NA - 1).astype(jnp.int32)
    expert_ids_keys = jax.random.split(jax.random.fold_in(key_list[2], 1), IMAGES * SEQ // TOK_DEV)
    expert_ids_turns = jax.random.permutation(jax.random.fold_in(key_list[2], 3), IMAGES * SEQ // TOK_DEV)
    expert_ids = jax.vmap(lambda own, number: assign_block(jax.random.fold_in(key_list[2], 2), own, number, TOK_DEV, E, TOPK, min(2 * CAP, TOK_DEV), 1))(expert_ids_keys, expert_ids_turns).reshape((IMAGES, SEQ, TOPK))
    cotangent = scatter_about(key_list[3], (IMAGES, SEQ, D), 1.0, 6.0, ((0, 32),))
    ln_gain1 = jnp.clip(1.0 + 0.18 * jax.random.normal(key_list[4], (D,), jnp.float32), 0.099609375, 1.8984375).astype(jnp.bfloat16)
    ln_gain2 = jnp.clip(1.0 + 0.18 * jax.random.normal(key_list[5], (D,), jnp.float32), 0.099609375, 1.8984375).astype(jnp.bfloat16)
    qkv_weight = scatter_about(key_list[6], (D, 3 * D), D ** -0.5, 0.25)
    out_weight = scatter_about(key_list[7], (D, D), (D // 16) ** -0.5, 1.0)
    router_weight = scatter_about(key_list[8], (D, E), (2 * D) ** -0.5, 0.1875)
    up_weight = scatter_about(key_list[9], (E, D, FF), D ** -0.5, 0.25, ((0, 4),))
    down_weight = scatter_about(key_list[10], (E, FF, D), FF ** -0.5, 0.125, ((0, 4),))
    qkv_a = scatter_about(key_list[11], (NA, D, R), D ** -0.5, 0.25)
    qkv_b = scatter_about(key_list[12], (NA, R, 3 * D), (2 * R) ** -0.5, 1.0)
    out_a = scatter_about(key_list[13], (NA, D, R), D ** -0.5, 0.25)
    out_b = scatter_about(key_list[14], (NA, R, D), (R // 4) ** -0.5, 3.0)
    router_a = scatter_about(key_list[15], (NA, D, R), D ** -0.5, 0.25)
    router_b = scatter_about(key_list[16], (NA, R, E), (4 * R) ** -0.5, 0.75)
    up_a = scatter_about(key_list[17], (E, NA, D, R), D ** -0.5, 0.25, ((0, 4),))
    up_b = scatter_about(key_list[18], (E, NA, R, FF), (2 * R) ** -0.5, 1.0, ((0, 4),))
    down_a = scatter_about(key_list[19], (E, NA, FF, R), FF ** -0.5, 0.125, ((0, 4),))
    down_b = scatter_about(key_list[20], (E, NA, R, D), (2 * R) ** -0.5, 1.0, ((0, 4),))
    return dict(images=images, adapter_ids=adapter_ids, expert_ids=expert_ids, cotangent=cotangent, ln_gain1=ln_gain1, ln_gain2=ln_gain2, qkv_weight=qkv_weight, out_weight=out_weight, router_weight=router_weight, up_weight=up_weight, down_weight=down_weight, qkv_a=qkv_a, qkv_b=qkv_b, out_a=out_a, out_b=out_b, router_a=router_a, router_b=router_b, up_a=up_a, up_b=up_b, down_a=down_a, down_b=down_b)


PRECISE = lax.Precision.HIGHEST
EPSILON = 1e-06

@jax.custom_vjp
def low(v):
    return lax.optimization_barrier(v.astype(jnp.bfloat16)).astype(jnp.float32)

@jax.custom_vjp
def low_back(v):
    return v

def low_keep(v):
    return (low(v), None)

def low_pass(kept, grad):
    return (grad,)

def back_keep(v):
    return (v, None)

def back_low(kept, grad):
    return (low(grad),)
low.defvjp(low_keep, low_pass)
low_back.defvjp(back_keep, back_low)

def layer_norm(values, gain):
    average = lax.optimization_barrier(jnp.mean(values, axis=-1, keepdims=True))
    centred = values - average
    spread = lax.optimization_barrier(jnp.mean(centred * centred, axis=-1, keepdims=True))
    return centred * lax.rsqrt(spread + EPSILON) * gain

def mixed(form, left, right):
    return jnp.einsum(form, left, right, precision=PRECISE, preferred_element_type=jnp.float32)

def take_rows(source, index):
    return source[index]

def placement_of(chosen):
    onehot = (chosen[:, :, None] == jnp.arange(E, dtype=jnp.int32)[None, None, :]).astype(jnp.int32)
    before = jnp.cumsum(onehot, axis=0, dtype=jnp.int32) - onehot
    first_total = lax.optimization_barrier(jnp.sum(onehot[:, 0], axis=0, dtype=jnp.int32))
    place_first = lax.optimization_barrier(jnp.sum(before[:, 0] * onehot[:, 0], axis=-1, dtype=jnp.int32))
    place_second = lax.optimization_barrier(jnp.sum((before[:, 1] + first_total[None, :]) * onehot[:, 1], axis=-1, dtype=jnp.int32))
    places = jnp.stack([place_first, place_second], axis=1)
    slot_index = jnp.where(places < CAP, chosen * CAP + places, E * CAP).astype(jnp.int32)
    owners = jnp.repeat(jnp.arange(TOK_DEV, dtype=jnp.int32), TOPK)
    slot_owner = jnp.full((E * CAP,), TOK_DEV, jnp.int32).at[slot_index.reshape(-1)].set(owners, mode='drop')
    return (slot_index, slot_owner)

def reference(images, adapter_ids, expert_ids, cotangent, ln_gain1, ln_gain2, qkv_weight, out_weight, router_weight, up_weight, down_weight, qkv_a, qkv_b, out_a, out_b, router_a, router_b, up_a, up_b, down_a, down_b):
    devices = N_DP * N_EXPERT
    gain_one = ln_gain1.astype(jnp.float32)
    gain_two = ln_gain2.astype(jnp.float32)
    qkv_base = qkv_weight.astype(jnp.float32)
    out_base = out_weight.astype(jnp.float32)
    router_base = router_weight.astype(jnp.float32)
    up_base = up_weight.astype(jnp.float32)
    down_base = down_weight.astype(jnp.float32)
    image_ids = adapter_ids.reshape(devices, IMG_DEV)
    chosen_ids = expert_ids.reshape(devices, TOK_DEV, TOPK)
    slot_index, slot_owner = jax.vmap(placement_of)(chosen_ids)
    token_ids = jnp.repeat(image_ids, SEQ, axis=1)
    padded_ids = jnp.concatenate([token_ids, jnp.zeros((devices, 1), jnp.int32)], axis=1)
    slot_ids = jax.vmap(take_rows)(padded_ids, slot_owner).reshape(devices, E, CAP).transpose(1, 0, 2)

    def forward(inputs, qkv_a, qkv_b, out_a, out_b, router_a, router_b, up_a, up_b, down_a, down_b):

        def attend(pair):
            block, block_ids = pair
            normed = low(layer_norm(block, gain_one))
            low_one = low_back(low(mixed('isd,idr->isr', normed, qkv_a[block_ids])))
            projected = mixed('isd,de->ise', normed, qkv_base) + mixed('isr,ire->ise', low_one, qkv_b[block_ids])
            projected = low_back(low(projected)).reshape(IMG_DEV, SEQ, 3, HEADS, HD)
            scores = low_back(mixed('ishd,ithd->ihst', projected[:, :, 0], projected[:, :, 1]) * (1.0 / math.sqrt(HD)))
            attention = low(jax.nn.softmax(scores, axis=-1))
            context = low_back(low(mixed('ihst,ithd->ishd', attention, projected[:, :, 2]))).reshape(IMG_DEV, SEQ, D)
            low_two = low_back(low(mixed('isd,idr->isr', context, out_a[block_ids])))
            branch = low_back(mixed('isd,de->ise', context, out_base) + mixed('isr,ire->ise', low_two, out_b[block_ids]))
            hidden_one = block + branch
            normed_two = low(layer_norm(hidden_one, gain_two))
            low_router = low_back(low(mixed('isd,idr->isr', normed_two, router_a[block_ids])))
            logits = low_back(mixed('isd,de->ise', normed_two, router_base) + mixed('isr,ire->ise', low_router, router_b[block_ids]))
            return (hidden_one.reshape(TOK_DEV, D), normed_two.reshape(TOK_DEV, D), logits.reshape(TOK_DEV, E))
        hidden_one, normed_two, logits = lax.map(jax.checkpoint(attend), (inputs, image_ids))
        chosen = jnp.take_along_axis(logits, chosen_ids, axis=-1)
        gates = jax.nn.softmax(chosen, axis=-1)
        padded_rows = jnp.concatenate([normed_two, jnp.zeros((devices, 1, D), jnp.float32)], axis=1)
        slot_rows = jax.vmap(take_rows)(padded_rows, slot_owner).reshape(devices, E, CAP, D).transpose(1, 0, 2, 3)

        def expert(pack):
            rows, row_ids, a_up, b_up, a_down, b_down, w_up, w_down = pack
            rows = low_back(rows)
            select = (row_ids[..., None] == jnp.arange(NA, dtype=jnp.int32)).astype(jnp.float32)[..., None]
            up_low = low_back(low(mixed('ncd,adr->ncar', rows, a_up))) * select
            preact = low_back(mixed('ncd,df->ncf', rows, w_up) + mixed('ncar,arf->ncf', up_low, b_up))
            hidden = low(jax.nn.gelu(preact, approximate=False))
            down_low = low_back(low(mixed('ncf,afr->ncar', hidden, a_down))) * select
            return low_back(low(mixed('ncf,fd->ncd', hidden, w_down) + mixed('ncar,ard->ncd', down_low, b_down)))
        outputs = lax.map(jax.checkpoint(expert), (slot_rows, slot_ids, up_a, up_b, down_a, down_b, up_base, down_base))
        outputs = outputs.transpose(1, 0, 2, 3).reshape(devices, E * CAP, D)
        padded_out = jnp.concatenate([outputs, jnp.zeros((devices, 1, D), jnp.float32)], axis=1)
        pair_out = jax.vmap(take_rows)(padded_out, slot_index)
        return hidden_one + lax.optimization_barrier(jnp.sum(gates[..., None] * pair_out, axis=2))
    inputs = images.astype(jnp.float32).reshape(devices, IMG_DEV, SEQ, D)
    result, pullback = jax.vjp(forward, inputs, qkv_a.astype(jnp.float32), qkv_b.astype(jnp.float32), out_a.astype(jnp.float32), out_b.astype(jnp.float32), router_a.astype(jnp.float32), router_b.astype(jnp.float32), up_a.astype(jnp.float32), up_b.astype(jnp.float32), down_a.astype(jnp.float32), down_b.astype(jnp.float32))
    grads = pullback(cotangent.astype(jnp.float32).reshape(devices, TOK_DEV, D))
    return (result.reshape(IMAGES, SEQ, D).astype(jnp.bfloat16), grads[0].reshape(IMAGES, SEQ, D), grads[1], grads[2], grads[3], grads[4], grads[5], grads[6], grads[7], grads[8], grads[9], grads[10])
```

```python
import functools

import jax
import jax.numpy as jnp
from jax import lax
from jax.experimental import pallas as pl
from jax.experimental.pallas import tpu as pltpu
from jax.sharding import PartitionSpec as P

HEADS = 8
EPSILON = 1e-06
F32 = jnp.float32
LOW = jnp.bfloat16
PIECES = 2
CHUNK = 512


def nn(left, right):
    return lax.dot_general(left, right, (((1,), (0,)), ((), ())), preferred_element_type=F32)


def nt(left, right):
    return lax.dot_general(left, right, (((1,), (1,)), ((), ())), preferred_element_type=F32)


def tn(left, right):
    return lax.dot_general(left, right, (((0,), (0,)), ((), ())), preferred_element_type=F32)


def normalise(values):
    average = jnp.mean(values, axis=-1, keepdims=True)
    centred = values - average
    spread = jnp.mean(centred * centred, axis=-1, keepdims=True)
    factor = lax.rsqrt(spread + EPSILON)
    return centred * factor, factor


def norm_back(grad, normed, factor, gain):
    scaled = grad * gain
    return factor * (
        scaled
        - jnp.mean(scaled, axis=-1, keepdims=True)
        - normed * jnp.mean(scaled * normed, axis=-1, keepdims=True)
    )


def soften(queries, keys, scale, real):
    scores = nt(queries, keys) * scale
    lanes = lax.broadcasted_iota(jnp.int32, scores.shape, 1)
    scores = jnp.where(lanes < real, scores, -1e30)
    powers = jnp.exp(scores - jnp.max(scores, axis=-1, keepdims=True))
    return powers * (1.0 / jnp.sum(powers, axis=-1, keepdims=True))


def pair_gates(first, second):
    top = jnp.maximum(first, second)
    one, two = jnp.exp(first - top), jnp.exp(second - top)
    total = 1.0 / (one + two)
    return one * total, two * total


def forward_kernel(
    real,
    ids_ref,
    images_ref,
    picks_ref,
    pick_rows_ref,
    gain1_ref,
    gain2_ref,
    wqkv_ref,
    wout_ref,
    wrouter_ref,
    qkv_a_ref,
    qkv_b_ref,
    out_a_ref,
    out_b_ref,
    router_a_ref,
    router_b_ref,
    qkv_ref,
    context_ref,
    hidden_ref,
    normed_ref,
    gates_ref,
    gate_rows_ref,
):
    width = images_ref.shape[2]
    size = width // HEADS
    scale = size ** (-0.5)
    inputs = images_ref[0].astype(F32)
    plain, _ = normalise(inputs)
    normed = (plain * gain1_ref[...]).astype(LOW)
    low_one = nt(normed, qkv_a_ref[0]).astype(LOW)
    qkv_ref[0] = (nn(normed, wqkv_ref[...]) + nn(low_one, qkv_b_ref[0])).astype(LOW)
    parts = []
    for head in range(HEADS):
        at = head * size
        probs = soften(
            qkv_ref[0, :, at : at + size],
            qkv_ref[0, :, width + at : width + at + size],
            scale,
            real,
        ).astype(LOW)
        values = qkv_ref[0, :, 2 * width + at : 2 * width + at + size]
        parts.append(nn(probs, values).astype(LOW))
    context = jnp.concatenate(parts, axis=1)
    context_ref[0] = context
    low_two = nt(context, out_a_ref[0]).astype(LOW)
    hidden = inputs + nn(context, wout_ref[...]) + nn(low_two, out_b_ref[0])
    hidden_ref[0] = hidden
    plain_two, _ = normalise(hidden)
    normed_two = (plain_two * gain2_ref[...]).astype(LOW)
    normed_ref[0] = normed_two
    low_router = nt(normed_two, router_a_ref[0]).astype(LOW)
    logits = nt(normed_two, wrouter_ref[...]) + nn(low_router, router_b_ref[0])
    lanes = lax.broadcasted_iota(jnp.int32, logits.shape, 1)
    chosen = [
        jnp.sum(jnp.where(lanes == picks_ref[0, :, k : k + 1], logits, 0.0), axis=1, keepdims=True)
        for k in range(2)
    ]
    gates_ref[0] = jnp.concatenate(pair_gates(*chosen), axis=1)
    low_rows = nt(router_a_ref[0], normed_two).astype(LOW)
    logit_rows = nt(wrouter_ref[...], normed_two) + tn(router_b_ref[0], low_rows)
    places = lax.broadcasted_iota(jnp.int32, logit_rows.shape, 0)
    chosen_rows = [
        jnp.sum(
            jnp.where(places == pick_rows_ref[0, k : k + 1, :], logit_rows, 0.0),
            axis=0,
            keepdims=True,
        )
        for k in range(2)
    ]
    gate_rows_ref[0] = jnp.concatenate(pair_gates(*chosen_rows), axis=0)


def gelu_pair(values):
    half = 0.5 * (1.0 + lax.erf(values * 0.7071067811865476))
    density = jnp.exp(values * values * -0.5) * 0.3989422804014327
    return values * half, half + values * density


def expert_kernel(
    n_here,
    first_ref,
    marks_ref,
    gate_rows_ref,
    tokens_ref,
    upstream_ref,
    up_ref,
    down_ref,
    up_a_ref,
    up_b_ref,
    down_a_ref,
    down_b_ref,
    back_ref,
    grads_ref,
    rows_ref,
    dy_ref,
    mask_ref,
    y_ref,
    dx_ref,
    low_ref,
    low_grad_ref,
    half_ref,
):
    groups, _, capacity, double = back_ref.shape
    width = double // 2
    ff_width = up_ref.shape[2]
    low_cols = up_a_ref.shape[1]
    rank = 16
    start = (first_ref[0] + pl.program_id(0)) * capacity
    for group in range(groups):
        span = slice(group * capacity, (group + 1) * capacity)
        n_tokens = tokens_ref.shape[1]
        slots = lax.broadcasted_iota(jnp.int32, (capacity, n_tokens), 0) + start
        zero = slots == marks_ref[group, 0:1, :]
        one = slots == marks_ref[group, 1:2, :]
        either = jnp.where(zero | one, 1.0, 0.0)
        gate = jnp.sum(
            jnp.where(zero, gate_rows_ref[group, 0:1, :], 0.0)
            + jnp.where(one, gate_rows_ref[group, 1:2, :], 0.0),
            axis=1,
            keepdims=True,
        )
        ids = jnp.sum(
            either * marks_ref[group, 2:3, :].astype(F32), axis=1, keepdims=True
        )
        either = either.astype(LOW)
        rows_ref[span, :] = nn(either, tokens_ref[group]).astype(LOW)
        dy_ref[span, :] = (gate * nn(either, upstream_ref[group])).astype(LOW)
        cols = lax.broadcasted_iota(jnp.int32, (capacity, low_cols), 1) // rank
        mask_ref[span, :] = jnp.where(cols.astype(F32) == ids, 1.0, 0.0)
    mask = mask_ref[...]
    up_low = (nt(rows_ref[...], up_a_ref[0]) * mask).astype(LOW)
    down_low_grad = (nt(dy_ref[...], down_b_ref[0]) * mask).astype(LOW)
    half_ref[0] = up_low.T
    half_ref[1] = down_low_grad.T
    y_ref[...] = jnp.zeros_like(y_ref)
    dx_ref[...] = jnp.zeros_like(dx_ref)
    low_ref[...] = jnp.zeros_like(low_ref)
    low_grad_ref[...] = jnp.zeros_like(low_grad_ref)
    up_b_at, down_a_at, down_b_at = width, width + ff_width, width + 2 * ff_width

    def step(number, carry):
        at = pl.multiple_of(number * CHUNK, CHUNK)
        cols = pl.ds(at, CHUNK)
        pre = nn(rows_ref[...], up_ref[0, :, cols]) + nn(up_low, up_b_ref[0, :, cols])
        hidden, slope = gelu_pair(pre)
        hidden = hidden.astype(LOW)
        grad = nt(dy_ref[...], down_ref[0, cols, :]) + nn(down_low_grad, down_a_ref[0, :, cols])
        grad = (grad * slope).astype(LOW)
        y_ref[...] += nn(hidden, down_ref[0, cols, :])
        low_ref[...] += nt(hidden, down_a_ref[0, :, cols])
        dx_ref[...] += nt(grad, up_ref[0, :, cols])
        low_grad_ref[...] += nt(grad, up_b_ref[0, :, cols])
        grads_ref[0, :, pl.ds(pl.multiple_of(up_b_at + at, CHUNK), CHUNK)] = nn(
            half_ref[0], grad
        ).astype(LOW)
        grads_ref[0, :, pl.ds(pl.multiple_of(down_a_at + at, CHUNK), CHUNK)] = nn(
            half_ref[1], hidden
        ).astype(LOW)
        return carry

    lax.fori_loop(0, ff_width // CHUNK, step, 0)
    down_low = (low_ref[...] * mask).astype(LOW)
    up_low_grad = (low_grad_ref[...] * mask).astype(LOW)
    out = (y_ref[...] + nn(down_low, down_b_ref[0])).astype(LOW)
    dx = (dx_ref[...] + nn(up_low_grad, up_a_ref[0])).astype(LOW)
    back_ref[:, 0, :, :width] = out.reshape(groups, capacity, width)
    back_ref[:, 0, :, width:] = dx.reshape(groups, capacity, width)
    grads_ref[0, :, 0:width] = tn(up_low_grad, rows_ref[...]).astype(LOW)
    grads_ref[0, :, down_b_at : down_b_at + width] = tn(down_low, dy_ref[...]).astype(LOW)


def backward_kernel(
    real,
    ids_ref,
    images_ref,
    upstream_ref,
    hidden_ref,
    normed_ref,
    qkv_ref,
    context_ref,
    gates_ref,
    picks_ref,
    slots_ref,
    gain1_ref,
    gain2_ref,
    wqkv_ref,
    wout_ref,
    wrouter_ref,
    qkv_a_ref,
    qkv_b_ref,
    out_a_ref,
    out_b_ref,
    router_a_ref,
    router_b_ref,
    *rest,
):
    back_refs = rest[:-5]
    out_ref, input_grad_ref, grads_ref, total_ref, dqkv_ref = rest[-5:]
    image = pl.program_id(0)
    own = ids_ref[image]
    width = images_ref.shape[2]
    size = width // HEADS
    scale = size ** (-0.5)
    n_experts = wrouter_ref.shape[0]

    @pl.when(image == 0)
    def _():
        total_ref[...] = jnp.zeros_like(total_ref)

    rows = images_ref.shape[1]
    pair_zero = pair_one = spread = None
    for number, back_ref in enumerate(back_refs):
        n_slots = back_ref.shape[0]
        slots = lax.broadcasted_iota(jnp.int32, (rows, n_slots), 1) + number * n_slots
        zero = jnp.where(slots == slots_ref[0, :, 0:1], 1.0, 0.0).astype(LOW)
        one = jnp.where(slots == slots_ref[0, :, 1:2], 1.0, 0.0).astype(LOW)
        terms = (
            nn(zero, back_ref[:, :width]),
            nn(one, back_ref[:, :width]),
            nn(zero + one, back_ref[:, width:]),
        )
        if number == 0:
            pair_zero, pair_one, spread = terms
        else:
            pair_zero, pair_one, spread = (
                pair_zero + terms[0],
                pair_one + terms[1],
                spread + terms[2],
            )
    gate_zero, gate_one = gates_ref[0, :, 0:1], gates_ref[0, :, 1:2]
    hidden = hidden_ref[0]
    out = (hidden + (gate_zero * pair_zero + gate_one * pair_one)).astype(LOW)
    out_ref[0] = out[:real]
    upstream = upstream_ref[0].astype(F32)
    grad_zero = jnp.sum(upstream * pair_zero, axis=1, keepdims=True)
    grad_one = jnp.sum(upstream * pair_one, axis=1, keepdims=True)
    centre = gate_zero * grad_zero + gate_one * grad_one
    lanes = lax.broadcasted_iota(jnp.int32, (rows, n_experts), 1)
    logits_grad = (
        jnp.where(lanes == picks_ref[0, :, 0:1], gate_zero * (grad_zero - centre), 0.0)
        + jnp.where(lanes == picks_ref[0, :, 1:2], gate_one * (grad_one - centre), 0.0)
    ).astype(LOW)
    normed_two = normed_ref[0]
    low_rows = nt(router_a_ref[0], normed_two).astype(LOW)
    router_low_grad = nt(logits_grad, router_b_ref[0]).astype(LOW)
    qkv_b_at, out_a_at, out_b_at = width, 4 * width, 5 * width
    router_a_at, router_b_at = 6 * width, 7 * width
    total_ref[own, :, router_b_at : router_b_at + n_experts] += nn(low_rows, logits_grad)
    total_ref[own, :, router_a_at : router_a_at + width] += tn(router_low_grad, normed_two)
    spread = spread + nn(logits_grad, wrouter_ref[...]) + nn(router_low_grad, router_a_ref[0])
    plain_two, factor_two = normalise(hidden)
    hidden_grad = upstream + norm_back(spread, plain_two, factor_two, gain2_ref[...])
    branch = hidden_grad.astype(LOW)
    context = context_ref[0]
    low_two = nt(context, out_a_ref[0]).astype(LOW)
    out_low_grad = nt(branch, out_b_ref[0]).astype(LOW)
    total_ref[own, :, out_b_at : out_b_at + width] += tn(low_two, branch)
    total_ref[own, :, out_a_at : out_a_at + width] += tn(out_low_grad, context)
    context_grad = (nt(branch, wout_ref[...]) + nn(out_low_grad, out_a_ref[0])).astype(LOW)
    for head in range(HEADS):
        at = head * size
        queries = qkv_ref[0, :, at : at + size]
        keys = qkv_ref[0, :, width + at : width + at + size]
        values = qkv_ref[0, :, 2 * width + at : 2 * width + at + size]
        own_grad = context_grad[:, at : at + size]
        probs = soften(queries, keys, scale, real)
        probs_grad = nt(own_grad, values)
        score_grad = (
            probs * (probs_grad - jnp.sum(probs_grad * probs, axis=-1, keepdims=True))
        ).astype(LOW)
        dqkv_ref[:, at : at + size] = (nn(score_grad, keys) * scale).astype(LOW)
        dqkv_ref[:, width + at : width + at + size] = (tn(score_grad, queries) * scale).astype(LOW)
        dqkv_ref[:, 2 * width + at : 2 * width + at + size] = tn(
            probs.astype(LOW), own_grad
        ).astype(LOW)
    plain, factor = normalise(images_ref[0].astype(F32))
    normed = (plain * gain1_ref[...]).astype(LOW)
    low_one = nt(normed, qkv_a_ref[0]).astype(LOW)
    dqkv = dqkv_ref[...]
    qkv_low_grad = nt(dqkv, qkv_b_ref[0]).astype(LOW)
    total_ref[own, :, qkv_b_at : qkv_b_at + 3 * width] += tn(low_one, dqkv)
    total_ref[own, :, 0:width] += tn(qkv_low_grad, normed)
    normed_grad = nt(dqkv, wqkv_ref[...]) + nn(qkv_low_grad, qkv_a_ref[0])
    input_grad = hidden_grad + norm_back(normed_grad, plain, factor, gain1_ref[...])
    input_grad_ref[0] = input_grad[:real]

    @pl.when(image == pl.num_programs(0) - 1)
    def _():
        grads_ref[...] = total_ref[...].astype(LOW)


def whole(array):
    rank = len(array.shape)
    return pl.BlockSpec(array.shape, lambda i, s: (0,) * rank)


def per_image(array):
    rank = len(array.shape)
    return pl.BlockSpec((1,) + array.shape[1:], lambda i, s: (i,) + (0,) * (rank - 1))


def per_adapter(array):
    rank = len(array.shape)
    return pl.BlockSpec((1,) + array.shape[1:], lambda i, s: (s[i],) + (0,) * (rank - 1))


def body(
    images,
    adapter_ids,
    expert_ids,
    cotangent,
    ln_gain1,
    ln_gain2,
    qkv_weight,
    out_weight,
    router_weight,
    up_weight,
    down_weight,
    qkv_a,
    qkv_b,
    out_a,
    out_b,
    router_a,
    router_b,
    up_a,
    up_b,
    down_a,
    down_b,
):
    n_images, seq_len, width = images.shape
    tokens = n_images * seq_len
    padded = -(-seq_len // 16) * 16
    rows = n_images * padded
    n_adapt, _, rank = qkv_a.shape
    low_cols = n_adapt * rank
    n_experts = router_weight.shape[1]
    local = up_weight.shape[0]
    ff_width = up_weight.shape[2]
    groups = lax.axis_size("expert")
    capacity = max(2, tokens * 2 * 5 // (4 * n_experts))
    room = -(-capacity // 16) * 16
    here = local // PIECES

    fill = ((0, 0), (0, padded - seq_len), (0, 0))
    images = jnp.pad(images, fill)
    upstream = jnp.pad(cotangent, fill)
    picks = jnp.pad(expert_ids, fill, constant_values=-1)
    pick_rows = picks.transpose(0, 2, 1)
    flat = pick_rows.transpose(1, 0, 2).reshape(2, rows)
    marks = flat[:, None, :] == jnp.arange(n_experts, dtype=jnp.int32)[None, :, None]
    order = jnp.arange(rows, dtype=jnp.int32)
    earlier = (order[:, None] < order[None, :]).astype(LOW)
    before = jnp.dot(
        marks.reshape(2 * n_experts, rows).astype(LOW), earlier, preferred_element_type=F32
    ).reshape(2, n_experts, rows)
    totals = jnp.sum(marks[0].astype(F32), axis=1)
    offset = jnp.stack([jnp.zeros_like(totals), totals])
    places = jnp.sum(
        jnp.where(marks, before + offset[:, :, None], 0.0), axis=1
    ).astype(jnp.int32)
    group_of, inner = flat // local, flat % local
    ranked = ((inner // here) * groups + group_of) * here + inner % here
    kept = (flat >= 0) & (places < capacity)
    slots = jnp.where(kept, ranked * room + places, -1)
    token_ids = jnp.broadcast_to(adapter_ids[:, None], (n_images, padded)).reshape(1, rows)
    slot_columns = slots.reshape(2, n_images, padded).transpose(1, 2, 0)
    side = jnp.concatenate([slots, token_ids], axis=0)
    side_all = lax.all_gather(side, "expert")
    upstream_all = lax.all_gather(upstream.reshape(rows, width), "expert")

    gain_one = ln_gain1.astype(F32).reshape(1, width)
    gain_two = ln_gain2.astype(F32).reshape(1, width)
    router_t = router_weight.T
    qkv_a_t = qkv_a.transpose(0, 2, 1)
    out_a_t = out_a.transpose(0, 2, 1)
    router_a_t = router_a.transpose(0, 2, 1)
    shared = (gain_one, gain_two, qkv_weight, out_weight, router_t)
    adapters = (qkv_a_t, qkv_b, out_a_t, out_b, router_a_t, router_b)
    grid_of = functools.partial(pltpu.PrefetchScalarGridSpec, num_scalar_prefetch=1)
    forward_out = (
        jax.ShapeDtypeStruct((n_images, padded, 3 * width), LOW),
        jax.ShapeDtypeStruct((n_images, padded, width), LOW),
        jax.ShapeDtypeStruct((n_images, padded, width), F32),
        jax.ShapeDtypeStruct((n_images, padded, width), LOW),
        jax.ShapeDtypeStruct((n_images, padded, 2), F32),
        jax.ShapeDtypeStruct((n_images, 2, padded), F32),
    )
    qkv, context, hidden, normed, gates, gate_rows = pl.pallas_call(
        functools.partial(forward_kernel, seq_len),
        out_shape=forward_out,
        grid_spec=grid_of(
            grid=(n_images,),
            in_specs=[per_image(a) for a in (images, picks, pick_rows)]
            + [whole(a) for a in shared]
            + [per_adapter(a) for a in adapters],
            out_specs=[per_image(a) for a in forward_out],
        ),
        name="attend",
    )(adapter_ids, images, picks, pick_rows, *shared, *adapters)

    normed_all = lax.all_gather(normed.reshape(rows, width), "expert")
    gates_all = lax.all_gather(gate_rows.transpose(1, 0, 2).reshape(2, rows), "expert")
    up_a_t = up_a.transpose(0, 1, 3, 2).reshape(local, low_cols, width)
    up_b_flat = up_b.reshape(local, low_cols, ff_width)
    down_a_t = down_a.transpose(0, 1, 3, 2).reshape(local, low_cols, ff_width)
    down_b_flat = down_b.reshape(local, low_cols, width)
    cols = 2 * width + 2 * ff_width
    backs, sums = [], []
    for piece in range(PIECES):
        at = piece * here

        def of_expert(array, at=at):
            rank = len(array.shape)
            return pl.BlockSpec(
                (1,) + array.shape[1:], lambda i, s: (i + at,) + (0,) * (rank - 1)
            )

        weights = (up_weight, down_weight, up_a_t, up_b_flat, down_a_t, down_b_flat)
        first = ((piece * groups + lax.axis_index("expert")) * here).astype(jnp.int32)
        gathered = (side_all, gates_all, normed_all, upstream_all)
        n_rows = groups * room
        back, grads = pl.pallas_call(
            functools.partial(expert_kernel, here),
            out_shape=(
                jax.ShapeDtypeStruct((groups, here, room, 2 * width), LOW),
                jax.ShapeDtypeStruct((here, low_cols, cols), LOW),
            ),
            grid_spec=grid_of(
                grid=(here,),
                in_specs=[whole(a) for a in gathered] + [of_expert(a) for a in weights],
                out_specs=[
                    pl.BlockSpec((groups, 1, room, 2 * width), lambda i, s: (0, i, 0, 0)),
                    pl.BlockSpec((1, low_cols, cols), lambda i, s: (i, 0, 0)),
                ],
                scratch_shapes=[
                    pltpu.VMEM((n_rows, width), LOW),
                    pltpu.VMEM((n_rows, width), LOW),
                    pltpu.VMEM((n_rows, low_cols), F32),
                    pltpu.VMEM((n_rows, width), F32),
                    pltpu.VMEM((n_rows, width), F32),
                    pltpu.VMEM((n_rows, low_cols), F32),
                    pltpu.VMEM((n_rows, low_cols), F32),
                    pltpu.VMEM((2, low_cols, n_rows), LOW),
                ],
            ),
            name=f"experts_{piece}",
        )(first.reshape(1), *gathered, *weights)
        backs.append(lax.all_to_all(back, "expert", split_axis=0, concat_axis=0, tiled=True))
        sums.append(lax.psum(grads, "dp"))
    backs = [back.reshape(groups * here * room, 2 * width) for back in backs]

    grad_cols = 7 * width + 128
    out_types = (
        jax.ShapeDtypeStruct((n_images, seq_len, width), LOW),
        jax.ShapeDtypeStruct((n_images, seq_len, width), F32),
        jax.ShapeDtypeStruct((n_adapt, rank, grad_cols), LOW),
    )
    by_image = (images, upstream, hidden, normed, qkv, context, gates, picks, slot_columns)
    block_out, input_grad, own_grads = pl.pallas_call(
        functools.partial(backward_kernel, seq_len),
        out_shape=out_types,
        grid_spec=grid_of(
            grid=(n_images,),
            in_specs=[per_image(a) for a in by_image]
            + [whole(a) for a in shared]
            + [per_adapter(a) for a in adapters]
            + [whole(a) for a in backs],
            out_specs=[per_image(out_types[0]), per_image(out_types[1]), whole(out_types[2])],
            scratch_shapes=[
                pltpu.VMEM((n_adapt, rank, grad_cols), F32),
                pltpu.VMEM((padded, 3 * width), LOW),
            ],
        ),
        name="attend_back",
    )(adapter_ids, *by_image, *shared, *adapters, *backs)
    own_grads = lax.psum(own_grads, ("dp", "expert")).astype(F32)
    grad_qkv_a = own_grads[:, :, :width].transpose(0, 2, 1)
    grad_qkv_b = own_grads[:, :, width : 4 * width]
    grad_out_a = own_grads[:, :, 4 * width : 5 * width].transpose(0, 2, 1)
    grad_out_b = own_grads[:, :, 5 * width : 6 * width]
    grad_router_a = own_grads[:, :, 6 * width : 7 * width].transpose(0, 2, 1)
    grad_router_b = own_grads[:, :, 7 * width : 7 * width + n_experts]

    def expert_part(start, length):
        parts = [total[:, :, start : start + length].astype(F32) for total in sums]
        return jnp.concatenate(parts, axis=0).reshape(local, n_adapt, rank, length)

    grad_up_a = expert_part(0, width).transpose(0, 1, 3, 2)
    grad_up_b = expert_part(width, ff_width)
    grad_down_a = expert_part(width + ff_width, ff_width).transpose(0, 1, 3, 2)
    grad_down_b = expert_part(width + 2 * ff_width, width)
    return (
        block_out,
        input_grad,
        grad_qkv_a,
        grad_qkv_b,
        grad_out_a,
        grad_out_b,
        grad_router_a,
        grad_router_b,
        grad_up_a,
        grad_up_b,
        grad_down_a,
        grad_down_b,
    )


def solution(mesh):
    tokens = P(("dp", "expert"), None, None)
    experts = P("expert", None, None, None)
    weights = P("expert", None, None)
    placed = (
        (tokens, P(("dp", "expert")), tokens, tokens)
        + (P(),) * 5
        + (weights,) * 2
        + (P(),) * 6
        + (experts,) * 4
    )
    return jax.shard_map(
        body,
        mesh=mesh,
        in_specs=placed,
        out_specs=(tokens, tokens) + (P(),) * 6 + (experts,) * 4,
        check_vma=False,
    )
```

```python
import functools

import jax
import jax.numpy as jnp
from jax import lax
from jax.experimental import pallas as pl
from jax.experimental.pallas import tpu as pltpu
from jax.sharding import PartitionSpec as P

HEADS = 8
EPSILON = 1e-06
F32 = jnp.float32
LOW = jnp.bfloat16
PIECES = 2
CHUNK = 512


def nn(left, right):
    return lax.dot_general(left, right, (((1,), (0,)), ((), ())), preferred_element_type=F32)


def nt(left, right):
    return lax.dot_general(left, right, (((1,), (1,)), ((), ())), preferred_element_type=F32)


def tn(left, right):
    return lax.dot_general(left, right, (((0,), (0,)), ((), ())), preferred_element_type=F32)


def normalise(values):
    average = jnp.mean(values, axis=-1, keepdims=True)
    centred = values - average
    spread = jnp.mean(centred * centred, axis=-1, keepdims=True)
    factor = lax.rsqrt(spread + EPSILON)
    return centred * factor, factor


def norm_back(grad, normed, factor, gain):
    scaled = grad * gain
    return factor * (
        scaled
        - jnp.mean(scaled, axis=-1, keepdims=True)
        - normed * jnp.mean(scaled * normed, axis=-1, keepdims=True)
    )


def soften(queries, keys, scale, real):
    scores = nt(queries, keys) * scale
    lanes = lax.broadcasted_iota(jnp.int32, scores.shape, 1)
    scores = jnp.where(lanes < real, scores, -1e30)
    powers = jnp.exp(scores - jnp.max(scores, axis=-1, keepdims=True))
    return powers * (1.0 / jnp.sum(powers, axis=-1, keepdims=True))


def pair_gates(first, second):
    top = jnp.maximum(first, second)
    one, two = jnp.exp(first - top), jnp.exp(second - top)
    total = 1.0 / (one + two)
    return one * total, two * total


def forward_kernel(
    real,
    ids_ref,
    images_ref,
    picks_ref,
    pick_rows_ref,
    gain1_ref,
    gain2_ref,
    wqkv_ref,
    wout_ref,
    wrouter_ref,
    qkv_a_ref,
    qkv_b_ref,
    out_a_ref,
    out_b_ref,
    router_a_ref,
    router_b_ref,
    qkv_ref,
    context_ref,
    hidden_ref,
    normed_ref,
    gates_ref,
    gate_rows_ref,
):
    width = images_ref.shape[2]
    size = width // HEADS
    scale = size ** (-0.5)
    inputs = images_ref[0].astype(F32)
    plain, _ = normalise(inputs)
    normed = (plain * gain1_ref[...]).astype(LOW)
    low_one = nt(normed, qkv_a_ref[0]).astype(LOW)
    qkv_ref[0] = (nn(normed, wqkv_ref[...]) + nn(low_one, qkv_b_ref[0])).astype(LOW)
    parts = []
    for head in range(HEADS):
        at = head * size
        probs = soften(
            qkv_ref[0, :, at : at + size],
            qkv_ref[0, :, width + at : width + at + size],
            scale,
            real,
        ).astype(LOW)
        values = qkv_ref[0, :, 2 * width + at : 2 * width + at + size]
        parts.append(nn(probs, values).astype(LOW))
    context = jnp.concatenate(parts, axis=1)
    context_ref[0] = context
    low_two = nt(context, out_a_ref[0]).astype(LOW)
    hidden = inputs + nn(context, wout_ref[...]) + nn(low_two, out_b_ref[0])
    hidden_ref[0] = hidden
    plain_two, _ = normalise(hidden)
    normed_two = (plain_two * gain2_ref[...]).astype(LOW)
    normed_ref[0] = normed_two
    low_router = nt(normed_two, router_a_ref[0]).astype(LOW)
    logits = nt(normed_two, wrouter_ref[...]) + nn(low_router, router_b_ref[0])
    lanes = lax.broadcasted_iota(jnp.int32, logits.shape, 1)
    chosen = [
        jnp.sum(jnp.where(lanes == picks_ref[0, :, k : k + 1], logits, 0.0), axis=1, keepdims=True)
        for k in range(2)
    ]
    gates_ref[0] = jnp.concatenate(pair_gates(*chosen), axis=1)
    low_rows = nt(router_a_ref[0], normed_two).astype(LOW)
    logit_rows = nt(wrouter_ref[...], normed_two) + tn(router_b_ref[0], low_rows)
    places = lax.broadcasted_iota(jnp.int32, logit_rows.shape, 0)
    chosen_rows = [
        jnp.sum(
            jnp.where(places == pick_rows_ref[0, k : k + 1, :], logit_rows, 0.0),
            axis=0,
            keepdims=True,
        )
        for k in range(2)
    ]
    gate_rows_ref[0] = jnp.concatenate(pair_gates(*chosen_rows), axis=0)


def gelu_pair(values):
    half = 0.5 * (1.0 + lax.erf(values * 0.7071067811865476))
    density = jnp.exp(values * values * -0.5) * 0.3989422804014327
    return values * half, half + values * density


def expert_kernel(
    n_here,
    first_ref,
    marks_ref,
    gate_rows_ref,
    tokens_ref,
    upstream_ref,
    up_ref,
    down_ref,
    up_a_ref,
    up_b_ref,
    down_a_ref,
    down_b_ref,
    back_ref,
    grads_ref,
    rows_ref,
    dy_ref,
    mask_ref,
    y_ref,
    dx_ref,
    low_ref,
    low_grad_ref,
    half_ref,
):
    groups, _, capacity, double = back_ref.shape
    width = double // 2
    ff_width = up_ref.shape[2]
    low_cols = up_a_ref.shape[1]
    rank = 16
    start = (first_ref[0] + pl.program_id(0)) * capacity
    for group in range(groups):
        span = slice(group * capacity, (group + 1) * capacity)
        n_tokens = tokens_ref.shape[1]
        slots = lax.broadcasted_iota(jnp.int32, (capacity, n_tokens), 0) + start
        zero = slots == marks_ref[group, 0:1, :]
        one = slots == marks_ref[group, 1:2, :]
        either = jnp.where(zero | one, 1.0, 0.0)
        gate = jnp.sum(
            jnp.where(zero, gate_rows_ref[group, 0:1, :], 0.0)
            + jnp.where(one, gate_rows_ref[group, 1:2, :], 0.0),
            axis=1,
            keepdims=True,
        )
        ids = jnp.sum(
            either * marks_ref[group, 2:3, :].astype(F32), axis=1, keepdims=True
        )
        either = either.astype(LOW)
        rows_ref[span, :] = nn(either, tokens_ref[group]).astype(LOW)
        dy_ref[span, :] = (gate * nn(either, upstream_ref[group])).astype(LOW)
        cols = lax.broadcasted_iota(jnp.int32, (capacity, low_cols), 1) // rank
        mask_ref[span, :] = jnp.where(cols.astype(F32) == ids, 1.0, 0.0)
    mask = mask_ref[...]
    up_low = (nt(rows_ref[...], up_a_ref[0]) * mask).astype(LOW)
    down_low_grad = (nt(dy_ref[...], down_b_ref[0]) * mask).astype(LOW)
    half_ref[0] = up_low.T
    half_ref[1] = down_low_grad.T
    y_ref[...] = jnp.zeros_like(y_ref)
    dx_ref[...] = jnp.zeros_like(dx_ref)
    low_ref[...] = jnp.zeros_like(low_ref)
    low_grad_ref[...] = jnp.zeros_like(low_grad_ref)
    up_b_at, down_a_at, down_b_at = width, width + ff_width, width + 2 * ff_width

    def step(number, carry):
        at = pl.multiple_of(number * CHUNK, CHUNK)
        cols = pl.ds(at, CHUNK)
        pre = nn(rows_ref[...], up_ref[0, :, cols]) + nn(up_low, up_b_ref[0, :, cols])
        hidden, slope = gelu_pair(pre)
        hidden = hidden.astype(LOW)
        grad = nt(dy_ref[...], down_ref[0, cols, :]) + nn(down_low_grad, down_a_ref[0, :, cols])
        grad = (grad * slope).astype(LOW)
        y_ref[...] += nn(hidden, down_ref[0, cols, :])
        low_ref[...] += nt(hidden, down_a_ref[0, :, cols])
        dx_ref[...] += nt(grad, up_ref[0, :, cols])
        low_grad_ref[...] += nt(grad, up_b_ref[0, :, cols])
        grads_ref[0, :, pl.ds(pl.multiple_of(up_b_at + at, CHUNK), CHUNK)] = nn(
            half_ref[0], grad
        ).astype(LOW)
        grads_ref[0, :, pl.ds(pl.multiple_of(down_a_at + at, CHUNK), CHUNK)] = nn(
            half_ref[1], hidden
        ).astype(LOW)
        return carry

    lax.fori_loop(0, ff_width // CHUNK, step, 0)
    down_low = (low_ref[...] * mask).astype(LOW)
    up_low_grad = (low_grad_ref[...] * mask).astype(LOW)
    out = (y_ref[...] + nn(down_low, down_b_ref[0])).astype(LOW)
    dx = (dx_ref[...] + nn(up_low_grad, up_a_ref[0])).astype(LOW)
    back_ref[:, 0, :, :width] = out.reshape(groups, capacity, width)
    back_ref[:, 0, :, width:] = dx.reshape(groups, capacity, width)
    grads_ref[0, :, 0:width] = tn(up_low_grad, rows_ref[...]).astype(LOW)
    grads_ref[0, :, down_b_at : down_b_at + width] = tn(down_low, dy_ref[...]).astype(LOW)


def backward_kernel(
    real,
    ids_ref,
    images_ref,
    upstream_ref,
    hidden_ref,
    normed_ref,
    qkv_ref,
    context_ref,
    gates_ref,
    picks_ref,
    slots_ref,
    gain1_ref,
    gain2_ref,
    wqkv_ref,
    wout_ref,
    wrouter_ref,
    qkv_a_ref,
    qkv_b_ref,
    out_a_ref,
    out_b_ref,
    router_a_ref,
    router_b_ref,
    *rest,
):
    back_refs = rest[:-5]
    out_ref, input_grad_ref, grads_ref, total_ref, dqkv_ref = rest[-5:]
    image = pl.program_id(0)
    own = ids_ref[image]
    width = images_ref.shape[2]
    size = width // HEADS
    scale = size ** (-0.5)
    n_experts = wrouter_ref.shape[0]

    @pl.when(image == 0)
    def _():
        total_ref[...] = jnp.zeros_like(total_ref)

    rows = images_ref.shape[1]
    pair_zero = pair_one = spread = None
    for number, back_ref in enumerate(back_refs):
        n_slots = back_ref.shape[0]
        slots = lax.broadcasted_iota(jnp.int32, (rows, n_slots), 1) + number * n_slots
        zero = jnp.where(slots == slots_ref[0, :, 0:1], 1.0, 0.0).astype(LOW)
        one = jnp.where(slots == slots_ref[0, :, 1:2], 1.0, 0.0).astype(LOW)
        terms = (
            nn(zero, back_ref[:, :width]),
            nn(one, back_ref[:, :width]),
            nn(zero + one, back_ref[:, width:]),
        )
        if number == 0:
            pair_zero, pair_one, spread = terms
        else:
            pair_zero, pair_one, spread = (
                pair_zero + terms[0],
                pair_one + terms[1],
                spread + terms[2],
            )
    gate_zero, gate_one = gates_ref[0, :, 0:1], gates_ref[0, :, 1:2]
    hidden = hidden_ref[0]
    out = (hidden + (gate_zero * pair_zero + gate_one * pair_one)).astype(LOW)
    out_ref[0] = out[:real]
    upstream = upstream_ref[0].astype(F32)
    grad_zero = jnp.sum(upstream * pair_zero, axis=1, keepdims=True)
    grad_one = jnp.sum(upstream * pair_one, axis=1, keepdims=True)
    centre = gate_zero * grad_zero + gate_one * grad_one
    lanes = lax.broadcasted_iota(jnp.int32, (rows, n_experts), 1)
    logits_grad = (
        jnp.where(lanes == picks_ref[0, :, 0:1], gate_zero * (grad_zero - centre), 0.0)
        + jnp.where(lanes == picks_ref[0, :, 1:2], gate_one * (grad_one - centre), 0.0)
    ).astype(LOW)
    normed_two = normed_ref[0]
    low_rows = nt(router_a_ref[0], normed_two).astype(LOW)
    router_low_grad = nt(logits_grad, router_b_ref[0]).astype(LOW)
    qkv_b_at, out_a_at, out_b_at = width, 4 * width, 5 * width
    router_a_at, router_b_at = 6 * width, 7 * width
    total_ref[own, :, router_b_at : router_b_at + n_experts] += nn(low_rows, logits_grad)
    total_ref[own, :, router_a_at : router_a_at + width] += tn(router_low_grad, normed_two)
    spread = spread + nn(logits_grad, wrouter_ref[...]) + nn(router_low_grad, router_a_ref[0])
    plain_two, factor_two = normalise(hidden)
    hidden_grad = upstream + norm_back(spread, plain_two, factor_two, gain2_ref[...])
    branch = hidden_grad.astype(LOW)
    context = context_ref[0]
    low_two = nt(context, out_a_ref[0]).astype(LOW)
    out_low_grad = nt(branch, out_b_ref[0]).astype(LOW)
    total_ref[own, :, out_b_at : out_b_at + width] += tn(low_two, branch)
    total_ref[own, :, out_a_at : out_a_at + width] += tn(out_low_grad, context)
    context_grad = (nt(branch, wout_ref[...]) + nn(out_low_grad, out_a_ref[0])).astype(LOW)
    for head in range(HEADS):
        at = head * size
        queries = qkv_ref[0, :, at : at + size]
        keys = qkv_ref[0, :, width + at : width + at + size]
        values = qkv_ref[0, :, 2 * width + at : 2 * width + at + size]
        own_grad = context_grad[:, at : at + size]
        probs = soften(queries, keys, scale, real)
        probs_grad = nt(own_grad, values)
        score_grad = (
            probs * (probs_grad - jnp.sum(probs_grad * probs, axis=-1, keepdims=True))
        ).astype(LOW)
        dqkv_ref[:, at : at + size] = (nn(score_grad, keys) * scale).astype(LOW)
        dqkv_ref[:, width + at : width + at + size] = (tn(score_grad, queries) * scale).astype(LOW)
        dqkv_ref[:, 2 * width + at : 2 * width + at + size] = tn(
            probs.astype(LOW), own_grad
        ).astype(LOW)
    plain, factor = normalise(images_ref[0].astype(F32))
    normed = (plain * gain1_ref[...]).astype(LOW)
    low_one = nt(normed, qkv_a_ref[0]).astype(LOW)
    dqkv = dqkv_ref[...]
    qkv_low_grad = nt(dqkv, qkv_b_ref[0]).astype(LOW)
    total_ref[own, :, qkv_b_at : qkv_b_at + 3 * width] += tn(low_one, dqkv)
    total_ref[own, :, 0:width] += tn(qkv_low_grad, normed)
    normed_grad = nt(dqkv, wqkv_ref[...]) + nn(qkv_low_grad, qkv_a_ref[0])
    input_grad = hidden_grad + norm_back(normed_grad, plain, factor, gain1_ref[...])
    input_grad_ref[0] = input_grad[:real]

    @pl.when(image == pl.num_programs(0) - 1)
    def _():
        for tile in range(total_ref.shape[2] // 128):
            grads_ref[:, tile] = total_ref[:, :, tile * 128 : tile * 128 + 128].astype(LOW)


def exchange_sum(values, axis):
    count = lax.axis_size(axis)
    parts = values.reshape(count, values.shape[0] // count, values.shape[1])
    parts = lax.all_to_all(parts, axis, split_axis=0, concat_axis=0, tiled=True)
    return jnp.sum(parts.astype(F32), axis=0).astype(LOW)


def exchange_gather(values, axis):
    count = lax.axis_size(axis)
    copies = jnp.broadcast_to(values[None], (count,) + values.shape)
    copies = lax.all_to_all(copies, axis, split_axis=0, concat_axis=0, tiled=True)
    return copies.reshape(count * values.shape[0], values.shape[1])


def sum_over_all(values):
    part = exchange_sum(exchange_sum(values, "expert"), "dp")
    return exchange_gather(exchange_gather(part, "dp"), "expert")


def sum_over_copies(values, split):
    if not split:
        return lax.psum(values, "dp")
    flat = values.reshape(-1, values.shape[-1])
    part = lax.psum_scatter(flat, "dp", scatter_dimension=0, tiled=True)
    return lax.all_gather(part, "dp", axis=0, tiled=True).reshape(values.shape)


def whole(array):
    rank = len(array.shape)
    return pl.BlockSpec(array.shape, lambda i, s: (0,) * rank)


def per_image(array):
    rank = len(array.shape)
    return pl.BlockSpec((1,) + array.shape[1:], lambda i, s: (i,) + (0,) * (rank - 1))


def per_adapter(array):
    rank = len(array.shape)
    return pl.BlockSpec((1,) + array.shape[1:], lambda i, s: (s[i],) + (0,) * (rank - 1))


def body(
    images,
    adapter_ids,
    expert_ids,
    cotangent,
    ln_gain1,
    ln_gain2,
    qkv_weight,
    out_weight,
    router_weight,
    up_weight,
    down_weight,
    qkv_a,
    qkv_b,
    out_a,
    out_b,
    router_a,
    router_b,
    up_a,
    up_b,
    down_a,
    down_b,
):
    n_images, seq_len, width = images.shape
    tokens = n_images * seq_len
    padded = -(-seq_len // 16) * 16
    rows = n_images * padded
    n_adapt, _, rank = qkv_a.shape
    low_cols = n_adapt * rank
    n_experts = router_weight.shape[1]
    local = up_weight.shape[0]
    ff_width = up_weight.shape[2]
    groups = lax.axis_size("expert")
    capacity = max(2, tokens * 2 * 5 // (4 * n_experts))
    room = -(-capacity // 16) * 16
    here = local // PIECES

    fill = ((0, 0), (0, padded - seq_len), (0, 0))
    images = jnp.pad(images, fill)
    upstream = jnp.pad(cotangent, fill)
    picks = jnp.pad(expert_ids, fill, constant_values=-1)
    pick_rows = picks.transpose(0, 2, 1)
    flat = pick_rows.transpose(1, 0, 2).reshape(2, rows)
    marks = flat[:, None, :] == jnp.arange(n_experts, dtype=jnp.int32)[None, :, None]
    order = jnp.arange(rows, dtype=jnp.int32)
    earlier = (order[:, None] < order[None, :]).astype(LOW)
    before = jnp.dot(
        marks.reshape(2 * n_experts, rows).astype(LOW), earlier, preferred_element_type=F32
    ).reshape(2, n_experts, rows)
    totals = jnp.sum(marks[0].astype(F32), axis=1)
    offset = jnp.stack([jnp.zeros_like(totals), totals])
    places = jnp.sum(
        jnp.where(marks, before + offset[:, :, None], 0.0), axis=1
    ).astype(jnp.int32)
    group_of, inner = flat // local, flat % local
    ranked = ((inner // here) * groups + group_of) * here + inner % here
    kept = (flat >= 0) & (places < capacity)
    slots = jnp.where(kept, ranked * room + places, -1)
    token_ids = jnp.broadcast_to(adapter_ids[:, None], (n_images, padded)).reshape(1, rows)
    slot_columns = slots.reshape(2, n_images, padded).transpose(1, 2, 0)
    side = jnp.concatenate([slots, token_ids], axis=0)
    side_all = lax.all_gather(side, "expert")
    upstream_all = lax.all_gather(upstream.reshape(rows, width), "expert")

    gain_one = ln_gain1.astype(F32).reshape(1, width)
    gain_two = ln_gain2.astype(F32).reshape(1, width)
    router_t = router_weight.T
    qkv_a_t = qkv_a.transpose(0, 2, 1)
    out_a_t = out_a.transpose(0, 2, 1)
    router_a_t = router_a.transpose(0, 2, 1)
    shared = (gain_one, gain_two, qkv_weight, out_weight, router_t)
    adapters = (qkv_a_t, qkv_b, out_a_t, out_b, router_a_t, router_b)
    grid_of = functools.partial(pltpu.PrefetchScalarGridSpec, num_scalar_prefetch=1)
    forward_out = (
        jax.ShapeDtypeStruct((n_images, padded, 3 * width), LOW),
        jax.ShapeDtypeStruct((n_images, padded, width), LOW),
        jax.ShapeDtypeStruct((n_images, padded, width), F32),
        jax.ShapeDtypeStruct((n_images, padded, width), LOW),
        jax.ShapeDtypeStruct((n_images, padded, 2), F32),
        jax.ShapeDtypeStruct((n_images, 2, padded), F32),
    )
    qkv, context, hidden, normed, gates, gate_rows = pl.pallas_call(
        functools.partial(forward_kernel, seq_len),
        out_shape=forward_out,
        grid_spec=grid_of(
            grid=(n_images,),
            in_specs=[per_image(a) for a in (images, picks, pick_rows)]
            + [whole(a) for a in shared]
            + [per_adapter(a) for a in adapters],
            out_specs=[per_image(a) for a in forward_out],
        ),
        name="attend",
    )(adapter_ids, images, picks, pick_rows, *shared, *adapters)

    normed_all = lax.all_gather(normed.reshape(rows, width), "expert")
    gates_all = lax.all_gather(gate_rows.transpose(1, 0, 2).reshape(2, rows), "expert")
    up_a_t = up_a.transpose(0, 1, 3, 2).reshape(local, low_cols, width)
    up_b_flat = up_b.reshape(local, low_cols, ff_width)
    down_a_t = down_a.transpose(0, 1, 3, 2).reshape(local, low_cols, ff_width)
    down_b_flat = down_b.reshape(local, low_cols, width)
    cols = 2 * width + 2 * ff_width
    backs, sums = [], []
    for piece in range(PIECES):
        at = piece * here

        def of_expert(array, at=at):
            rank = len(array.shape)
            return pl.BlockSpec(
                (1,) + array.shape[1:], lambda i, s: (i + at,) + (0,) * (rank - 1)
            )

        weights = (up_weight, down_weight, up_a_t, up_b_flat, down_a_t, down_b_flat)
        first = ((piece * groups + lax.axis_index("expert")) * here).astype(jnp.int32)
        gathered = (side_all, gates_all, normed_all, upstream_all)
        n_rows = groups * room
        back, grads = pl.pallas_call(
            functools.partial(expert_kernel, here),
            out_shape=(
                jax.ShapeDtypeStruct((groups, here, room, 2 * width), LOW),
                jax.ShapeDtypeStruct((here, low_cols, cols), LOW),
            ),
            grid_spec=grid_of(
                grid=(here,),
                in_specs=[whole(a) for a in gathered] + [of_expert(a) for a in weights],
                out_specs=[
                    pl.BlockSpec((groups, 1, room, 2 * width), lambda i, s: (0, i, 0, 0)),
                    pl.BlockSpec((1, low_cols, cols), lambda i, s: (i, 0, 0)),
                ],
                scratch_shapes=[
                    pltpu.VMEM((n_rows, width), LOW),
                    pltpu.VMEM((n_rows, width), LOW),
                    pltpu.VMEM((n_rows, low_cols), F32),
                    pltpu.VMEM((n_rows, width), F32),
                    pltpu.VMEM((n_rows, width), F32),
                    pltpu.VMEM((n_rows, low_cols), F32),
                    pltpu.VMEM((n_rows, low_cols), F32),
                    pltpu.VMEM((2, low_cols, n_rows), LOW),
                ],
            ),
            name=f"experts_{piece}",
        )(first.reshape(1), *gathered, *weights)
        backs.append(lax.all_to_all(back, "expert", split_axis=0, concat_axis=0, tiled=True))
        sums.append(sum_over_copies(grads, piece > 0))
    backs = [back.reshape(groups * here * room, 2 * width) for back in backs]

    grad_cols = 8 * width
    tiles = grad_cols // 128
    out_types = (
        jax.ShapeDtypeStruct((n_images, seq_len, width), LOW),
        jax.ShapeDtypeStruct((n_images, seq_len, width), F32),
        jax.ShapeDtypeStruct((n_adapt, tiles, rank, 128), LOW),
    )
    by_image = (images, upstream, hidden, normed, qkv, context, gates, picks, slot_columns)
    block_out, input_grad, own_grads = pl.pallas_call(
        functools.partial(backward_kernel, seq_len),
        out_shape=out_types,
        grid_spec=grid_of(
            grid=(n_images,),
            in_specs=[per_image(a) for a in by_image]
            + [whole(a) for a in shared]
            + [per_adapter(a) for a in adapters]
            + [whole(a) for a in backs],
            out_specs=[per_image(out_types[0]), per_image(out_types[1]), whole(out_types[2])],
            scratch_shapes=[
                pltpu.VMEM((n_adapt, rank, grad_cols), F32),
                pltpu.VMEM((padded, 3 * width), LOW),
            ],
        ),
        name="attend_back",
    )(adapter_ids, *by_image, *shared, *adapters, *backs)
    own_grads = sum_over_all(own_grads.reshape(-1, 128)).reshape(n_adapt, tiles, rank, 128)

    def own_part(start, length):
        part = own_grads[:, start // 128 : -(-(start + length) // 128)].astype(F32)
        return part.transpose(0, 2, 1, 3).reshape(n_adapt, rank, -1)[:, :, :length]

    grad_qkv_a = own_part(0, width).transpose(0, 2, 1)
    grad_qkv_b = own_part(width, 3 * width)
    grad_out_a = own_part(4 * width, width).transpose(0, 2, 1)
    grad_out_b = own_part(5 * width, width)
    grad_router_a = own_part(6 * width, width).transpose(0, 2, 1)
    grad_router_b = own_part(7 * width, n_experts)

    def expert_part(start, length):
        parts = [total[:, :, start : start + length].astype(F32) for total in sums]
        return jnp.concatenate(parts, axis=0).reshape(local, n_adapt, rank, length)

    grad_up_a = expert_part(0, width).transpose(0, 1, 3, 2)
    grad_up_b = expert_part(width, ff_width)
    grad_down_a = expert_part(width + ff_width, ff_width).transpose(0, 1, 3, 2)
    grad_down_b = expert_part(width + 2 * ff_width, width)
    return (
        block_out,
        input_grad,
        grad_qkv_a,
        grad_qkv_b,
        grad_out_a,
        grad_out_b,
        grad_router_a,
        grad_router_b,
        grad_up_a,
        grad_up_b,
        grad_down_a,
        grad_down_b,
    )


def solution(mesh):
    tokens = P(("dp", "expert"), None, None)
    experts = P("expert", None, None, None)
    weights = P("expert", None, None)
    placed = (
        (tokens, P(("dp", "expert")), tokens, tokens)
        + (P(),) * 5
        + (weights,) * 2
        + (P(),) * 6
        + (experts,) * 4
    )
    return jax.shard_map(
        body,
        mesh=mesh,
        in_specs=placed,
        out_specs=(tokens, tokens) + (P(),) * 6 + (experts,) * 4,
        check_vma=False,
    )
```

```python
import functools

import jax
import jax.numpy as jnp
from jax import lax
from jax.experimental import pallas as pl
from jax.experimental.pallas import tpu as pltpu
from jax.sharding import PartitionSpec as P

HEADS = 8
EPSILON = 1e-06
F32 = jnp.float32
LOW = jnp.bfloat16
PIECES = 2
CHUNK = 512


def nn(left, right):
    return lax.dot_general(left, right, (((1,), (0,)), ((), ())), preferred_element_type=F32)


def nt(left, right):
    return lax.dot_general(left, right, (((1,), (1,)), ((), ())), preferred_element_type=F32)


def tn(left, right):
    return lax.dot_general(left, right, (((0,), (0,)), ((), ())), preferred_element_type=F32)


def normalise(values):
    average = jnp.mean(values, axis=-1, keepdims=True)
    centred = values - average
    spread = jnp.mean(centred * centred, axis=-1, keepdims=True)
    factor = lax.rsqrt(spread + EPSILON)
    return centred * factor, factor


def norm_back(grad, normed, factor, gain):
    scaled = grad * gain
    return factor * (
        scaled
        - jnp.mean(scaled, axis=-1, keepdims=True)
        - normed * jnp.mean(scaled * normed, axis=-1, keepdims=True)
    )


def soften(queries, keys, scale, real):
    scores = nt(queries, keys) * scale
    lanes = lax.broadcasted_iota(jnp.int32, scores.shape, 1)
    scores = jnp.where(lanes < real, scores, -1e30)
    powers = jnp.exp(scores - jnp.max(scores, axis=-1, keepdims=True))
    return powers * (1.0 / jnp.sum(powers, axis=-1, keepdims=True))


def pair_gates(first, second):
    top = jnp.maximum(first, second)
    one, two = jnp.exp(first - top), jnp.exp(second - top)
    total = 1.0 / (one + two)
    return one * total, two * total


def forward_kernel(
    real,
    ids_ref,
    images_ref,
    picks_ref,
    pick_rows_ref,
    gain1_ref,
    gain2_ref,
    wqkv_ref,
    wout_ref,
    wrouter_ref,
    qkv_a_ref,
    qkv_b_ref,
    out_a_ref,
    out_b_ref,
    router_a_ref,
    router_b_ref,
    qkv_ref,
    context_ref,
    hidden_ref,
    normed_ref,
    gates_ref,
    gate_rows_ref,
):
    width = images_ref.shape[2]
    size = width // HEADS
    scale = size ** (-0.5)
    inputs = images_ref[0].astype(F32)
    plain, _ = normalise(inputs)
    normed = (plain * gain1_ref[...]).astype(LOW)
    low_one = nt(normed, qkv_a_ref[0]).astype(LOW)
    qkv_ref[0] = (nn(normed, wqkv_ref[...]) + nn(low_one, qkv_b_ref[0])).astype(LOW)
    parts = []
    for head in range(HEADS):
        at = head * size
        probs = soften(
            qkv_ref[0, :, at : at + size],
            qkv_ref[0, :, width + at : width + at + size],
            scale,
            real,
        ).astype(LOW)
        values = qkv_ref[0, :, 2 * width + at : 2 * width + at + size]
        parts.append(nn(probs, values).astype(LOW))
    context = jnp.concatenate(parts, axis=1)
    context_ref[0] = context
    low_two = nt(context, out_a_ref[0]).astype(LOW)
    hidden = inputs + nn(context, wout_ref[...]) + nn(low_two, out_b_ref[0])
    hidden_ref[0] = hidden
    plain_two, _ = normalise(hidden)
    normed_two = (plain_two * gain2_ref[...]).astype(LOW)
    normed_ref[0] = normed_two
    low_router = nt(normed_two, router_a_ref[0]).astype(LOW)
    logits = nt(normed_two, wrouter_ref[...]) + nn(low_router, router_b_ref[0])
    lanes = lax.broadcasted_iota(jnp.int32, logits.shape, 1)
    chosen = [
        jnp.sum(jnp.where(lanes == picks_ref[0, :, k : k + 1], logits, 0.0), axis=1, keepdims=True)
        for k in range(2)
    ]
    gates_ref[0] = jnp.concatenate(pair_gates(*chosen), axis=1)
    low_rows = nt(router_a_ref[0], normed_two).astype(LOW)
    logit_rows = nt(wrouter_ref[...], normed_two) + tn(router_b_ref[0], low_rows)
    places = lax.broadcasted_iota(jnp.int32, logit_rows.shape, 0)
    chosen_rows = [
        jnp.sum(
            jnp.where(places == pick_rows_ref[0, k : k + 1, :], logit_rows, 0.0),
            axis=0,
            keepdims=True,
        )
        for k in range(2)
    ]
    gate_rows_ref[0] = jnp.concatenate(pair_gates(*chosen_rows), axis=0)


def gelu_pair(values):
    half = 0.5 * (1.0 + lax.erf(values * 0.7071067811865476))
    density = jnp.exp(values * values * -0.5) * 0.3989422804014327
    return values * half, half + values * density


def expert_kernel(
    n_after,
    first_ref,
    marks_ref,
    gate_rows_ref,
    tokens_ref,
    upstream_ref,
    up_ref,
    down_ref,
    up_a_ref,
    up_b_ref,
    down_a_ref,
    down_b_ref,
    *rest,
):
    back_ref, grads_ref, rows_ref, dy_ref, mask_ref = rest[n_after : n_after + 5]
    y_ref, dx_ref, low_ref, low_grad_ref, half_ref = rest[n_after + 5 :]
    groups, _, capacity, double = back_ref.shape
    width = double // 2
    ff_width = up_ref.shape[2]
    low_cols = up_a_ref.shape[1]
    rank = 16
    start = (first_ref[0] + pl.program_id(0)) * capacity
    for group in range(groups):
        span = slice(group * capacity, (group + 1) * capacity)
        n_tokens = tokens_ref.shape[1]
        slots = lax.broadcasted_iota(jnp.int32, (capacity, n_tokens), 0) + start
        zero = slots == marks_ref[group, 0:1, :]
        one = slots == marks_ref[group, 1:2, :]
        either = jnp.where(zero | one, 1.0, 0.0)
        gate = jnp.sum(
            jnp.where(zero, gate_rows_ref[group, 0:1, :], 0.0)
            + jnp.where(one, gate_rows_ref[group, 1:2, :], 0.0),
            axis=1,
            keepdims=True,
        )
        ids = jnp.sum(
            either * marks_ref[group, 2:3, :].astype(F32), axis=1, keepdims=True
        )
        either = either.astype(LOW)
        rows_ref[span, :] = nn(either, tokens_ref[group]).astype(LOW)
        dy_ref[span, :] = (gate * nn(either, upstream_ref[group])).astype(LOW)
        cols = lax.broadcasted_iota(jnp.int32, (capacity, low_cols), 1) // rank
        mask_ref[span, :] = jnp.where(cols.astype(F32) == ids, 1.0, 0.0)
    mask = mask_ref[...]
    up_low = (nt(rows_ref[...], up_a_ref[0]) * mask).astype(LOW)
    down_low_grad = (nt(dy_ref[...], down_b_ref[0]) * mask).astype(LOW)
    half_ref[0] = up_low.T
    half_ref[1] = down_low_grad.T
    y_ref[...] = jnp.zeros_like(y_ref)
    dx_ref[...] = jnp.zeros_like(dx_ref)
    low_ref[...] = jnp.zeros_like(low_ref)
    low_grad_ref[...] = jnp.zeros_like(low_grad_ref)
    up_b_at, down_a_at, down_b_at = width, width + ff_width, width + 2 * ff_width

    def step(number, carry):
        at = pl.multiple_of(number * CHUNK, CHUNK)
        cols = pl.ds(at, CHUNK)
        pre = nn(rows_ref[...], up_ref[0, :, cols]) + nn(up_low, up_b_ref[0, :, cols])
        hidden, slope = gelu_pair(pre)
        hidden = hidden.astype(LOW)
        grad = nt(dy_ref[...], down_ref[0, cols, :]) + nn(down_low_grad, down_a_ref[0, :, cols])
        grad = (grad * slope).astype(LOW)
        y_ref[...] += nn(hidden, down_ref[0, cols, :])
        low_ref[...] += nt(hidden, down_a_ref[0, :, cols])
        dx_ref[...] += nt(grad, up_ref[0, :, cols])
        low_grad_ref[...] += nt(grad, up_b_ref[0, :, cols])
        grads_ref[0, :, pl.ds(pl.multiple_of(up_b_at + at, CHUNK), CHUNK)] = nn(
            half_ref[0], grad
        ).astype(LOW)
        grads_ref[0, :, pl.ds(pl.multiple_of(down_a_at + at, CHUNK), CHUNK)] = nn(
            half_ref[1], hidden
        ).astype(LOW)
        return carry

    lax.fori_loop(0, ff_width // CHUNK, step, 0)
    down_low = (low_ref[...] * mask).astype(LOW)
    up_low_grad = (low_grad_ref[...] * mask).astype(LOW)
    out = (y_ref[...] + nn(down_low, down_b_ref[0])).astype(LOW)
    dx = (dx_ref[...] + nn(up_low_grad, up_a_ref[0])).astype(LOW)
    back_ref[:, 0, :, :width] = out.reshape(groups, capacity, width)
    back_ref[:, 0, :, width:] = dx.reshape(groups, capacity, width)
    grads_ref[0, :, 0:width] = tn(up_low_grad, rows_ref[...]).astype(LOW)
    grads_ref[0, :, down_b_at : down_b_at + width] = tn(down_low, dy_ref[...]).astype(LOW)


def backward_kernel(
    real,
    ids_ref,
    images_ref,
    upstream_ref,
    hidden_ref,
    normed_ref,
    qkv_ref,
    context_ref,
    gates_ref,
    picks_ref,
    slots_ref,
    gain1_ref,
    gain2_ref,
    wqkv_ref,
    wout_ref,
    wrouter_ref,
    qkv_a_ref,
    qkv_b_ref,
    out_a_ref,
    out_b_ref,
    router_a_ref,
    router_b_ref,
    *rest,
):
    back_refs = rest[:-5]
    out_ref, input_grad_ref, grads_ref, total_ref, dqkv_ref = rest[-5:]
    image = pl.program_id(0)
    own = ids_ref[image]
    width = images_ref.shape[2]
    size = width // HEADS
    scale = size ** (-0.5)
    n_experts = wrouter_ref.shape[0]

    @pl.when(image == 0)
    def _():
        total_ref[...] = jnp.zeros_like(total_ref)

    rows = images_ref.shape[1]
    pair_zero = pair_one = spread = None
    for number, back_ref in enumerate(back_refs):
        n_slots = back_ref.shape[0]
        slots = lax.broadcasted_iota(jnp.int32, (rows, n_slots), 1) + number * n_slots
        zero = jnp.where(slots == slots_ref[0, :, 0:1], 1.0, 0.0).astype(LOW)
        one = jnp.where(slots == slots_ref[0, :, 1:2], 1.0, 0.0).astype(LOW)
        terms = (
            nn(zero, back_ref[:, :width]),
            nn(one, back_ref[:, :width]),
            nn(zero + one, back_ref[:, width:]),
        )
        if number == 0:
            pair_zero, pair_one, spread = terms
        else:
            pair_zero, pair_one, spread = (
                pair_zero + terms[0],
                pair_one + terms[1],
                spread + terms[2],
            )
    gate_zero, gate_one = gates_ref[0, :, 0:1], gates_ref[0, :, 1:2]
    hidden = hidden_ref[0]
    out = (hidden + (gate_zero * pair_zero + gate_one * pair_one)).astype(LOW)
    out_ref[0] = out[:real]
    upstream = upstream_ref[0].astype(F32)
    grad_zero = jnp.sum(upstream * pair_zero, axis=1, keepdims=True)
    grad_one = jnp.sum(upstream * pair_one, axis=1, keepdims=True)
    centre = gate_zero * grad_zero + gate_one * grad_one
    lanes = lax.broadcasted_iota(jnp.int32, (rows, n_experts), 1)
    logits_grad = (
        jnp.where(lanes == picks_ref[0, :, 0:1], gate_zero * (grad_zero - centre), 0.0)
        + jnp.where(lanes == picks_ref[0, :, 1:2], gate_one * (grad_one - centre), 0.0)
    ).astype(LOW)
    normed_two = normed_ref[0]
    low_rows = nt(router_a_ref[0], normed_two).astype(LOW)
    router_low_grad = nt(logits_grad, router_b_ref[0]).astype(LOW)
    qkv_b_at, out_a_at, out_b_at = width, 4 * width, 5 * width
    router_a_at, router_b_at = 6 * width, 7 * width
    total_ref[own, :, router_b_at : router_b_at + n_experts] += nn(low_rows, logits_grad)
    total_ref[own, :, router_a_at : router_a_at + width] += tn(router_low_grad, normed_two)
    spread = spread + nn(logits_grad, wrouter_ref[...]) + nn(router_low_grad, router_a_ref[0])
    plain_two, factor_two = normalise(hidden)
    hidden_grad = upstream + norm_back(spread, plain_two, factor_two, gain2_ref[...])
    branch = hidden_grad.astype(LOW)
    context = context_ref[0]
    low_two = nt(context, out_a_ref[0]).astype(LOW)
    out_low_grad = nt(branch, out_b_ref[0]).astype(LOW)
    total_ref[own, :, out_b_at : out_b_at + width] += tn(low_two, branch)
    total_ref[own, :, out_a_at : out_a_at + width] += tn(out_low_grad, context)
    context_grad = (nt(branch, wout_ref[...]) + nn(out_low_grad, out_a_ref[0])).astype(LOW)
    for head in range(HEADS):
        at = head * size
        queries = qkv_ref[0, :, at : at + size]
        keys = qkv_ref[0, :, width + at : width + at + size]
        values = qkv_ref[0, :, 2 * width + at : 2 * width + at + size]
        own_grad = context_grad[:, at : at + size]
        probs = soften(queries, keys, scale, real)
        probs_grad = nt(own_grad, values)
        score_grad = (
            probs * (probs_grad - jnp.sum(probs_grad * probs, axis=-1, keepdims=True))
        ).astype(LOW)
        dqkv_ref[:, at : at + size] = (nn(score_grad, keys) * scale).astype(LOW)
        dqkv_ref[:, width + at : width + at + size] = (tn(score_grad, queries) * scale).astype(LOW)
        dqkv_ref[:, 2 * width + at : 2 * width + at + size] = tn(
            probs.astype(LOW), own_grad
        ).astype(LOW)
    plain, factor = normalise(images_ref[0].astype(F32))
    normed = (plain * gain1_ref[...]).astype(LOW)
    low_one = nt(normed, qkv_a_ref[0]).astype(LOW)
    dqkv = dqkv_ref[...]
    qkv_low_grad = nt(dqkv, qkv_b_ref[0]).astype(LOW)
    total_ref[own, :, qkv_b_at : qkv_b_at + 3 * width] += tn(low_one, dqkv)
    total_ref[own, :, 0:width] += tn(qkv_low_grad, normed)
    normed_grad = nt(dqkv, wqkv_ref[...]) + nn(qkv_low_grad, qkv_a_ref[0])
    input_grad = hidden_grad + norm_back(normed_grad, plain, factor, gain1_ref[...])
    input_grad_ref[0] = input_grad[:real]

    @pl.when(image == pl.num_programs(0) - 1)
    def _():
        for tile in range(total_ref.shape[2] // 128):
            grads_ref[:, tile] = total_ref[:, :, tile * 128 : tile * 128 + 128].astype(LOW)


def exchange_sum(values, axis):
    count = lax.axis_size(axis)
    parts = values.reshape(count, values.shape[0] // count, values.shape[1])
    parts = lax.all_to_all(parts, axis, split_axis=0, concat_axis=0, tiled=True)
    return jnp.sum(parts.astype(F32), axis=0).astype(LOW)


def exchange_gather(values, axis):
    count = lax.axis_size(axis)
    copies = jnp.broadcast_to(values[None], (count,) + values.shape)
    copies = lax.all_to_all(copies, axis, split_axis=0, concat_axis=0, tiled=True)
    return copies.reshape(count * values.shape[0], values.shape[1])


def sum_over_all(values):
    part = exchange_sum(exchange_sum(values, "expert"), "dp")
    return exchange_gather(exchange_gather(part, "dp"), "expert")


def sum_over_copies(values, split):
    if not split:
        return lax.psum(values, "dp")
    flat = values.reshape(-1, values.shape[-1])
    part = exchange_sum(flat, "dp")
    return lax.all_gather(part, "dp", axis=0, tiled=True).reshape(values.shape)


def work_of(microseconds):
    return pl.CostEstimate(flops=microseconds * 10**9, bytes_accessed=10**6, transcendentals=0)


def whole(array):
    rank = len(array.shape)
    return pl.BlockSpec(array.shape, lambda i, s: (0,) * rank)


def per_image(array):
    rank = len(array.shape)
    return pl.BlockSpec((1,) + array.shape[1:], lambda i, s: (i,) + (0,) * (rank - 1))


def per_adapter(array):
    rank = len(array.shape)
    return pl.BlockSpec((1,) + array.shape[1:], lambda i, s: (s[i],) + (0,) * (rank - 1))


def body(
    images,
    adapter_ids,
    expert_ids,
    cotangent,
    ln_gain1,
    ln_gain2,
    qkv_weight,
    out_weight,
    router_weight,
    up_weight,
    down_weight,
    qkv_a,
    qkv_b,
    out_a,
    out_b,
    router_a,
    router_b,
    up_a,
    up_b,
    down_a,
    down_b,
):
    n_images, seq_len, width = images.shape
    tokens = n_images * seq_len
    padded = -(-seq_len // 16) * 16
    rows = n_images * padded
    n_adapt, _, rank = qkv_a.shape
    low_cols = n_adapt * rank
    n_experts = router_weight.shape[1]
    local = up_weight.shape[0]
    ff_width = up_weight.shape[2]
    groups = lax.axis_size("expert")
    capacity = max(2, tokens * 2 * 5 // (4 * n_experts))
    room = -(-capacity // 16) * 16
    here = local // PIECES

    fill = ((0, 0), (0, padded - seq_len), (0, 0))
    images = jnp.pad(images, fill)
    upstream = jnp.pad(cotangent, fill)
    picks = jnp.pad(expert_ids, fill, constant_values=-1)
    pick_rows = picks.transpose(0, 2, 1)
    flat = pick_rows.transpose(1, 0, 2).reshape(2, rows)
    marks = flat[:, None, :] == jnp.arange(n_experts, dtype=jnp.int32)[None, :, None]
    order = jnp.arange(rows, dtype=jnp.int32)
    earlier = (order[:, None] < order[None, :]).astype(LOW)
    before = jnp.dot(
        marks.reshape(2 * n_experts, rows).astype(LOW), earlier, preferred_element_type=F32
    ).reshape(2, n_experts, rows)
    totals = jnp.sum(marks[0].astype(F32), axis=1)
    offset = jnp.stack([jnp.zeros_like(totals), totals])
    places = jnp.sum(
        jnp.where(marks, before + offset[:, :, None], 0.0), axis=1
    ).astype(jnp.int32)
    group_of, inner = flat // local, flat % local
    ranked = ((inner // here) * groups + group_of) * here + inner % here
    kept = (flat >= 0) & (places < capacity)
    slots = jnp.where(kept, ranked * room + places, -1)
    token_ids = jnp.broadcast_to(adapter_ids[:, None], (n_images, padded)).reshape(1, rows)
    slot_columns = slots.reshape(2, n_images, padded).transpose(1, 2, 0)
    side = jnp.concatenate([slots, token_ids], axis=0)
    side_all = lax.all_gather(side, "expert")
    upstream_all = lax.all_gather(upstream.reshape(rows, width), "expert")

    gain_one = ln_gain1.astype(F32).reshape(1, width)
    gain_two = ln_gain2.astype(F32).reshape(1, width)
    router_t = router_weight.T
    qkv_a_t = qkv_a.transpose(0, 2, 1)
    out_a_t = out_a.transpose(0, 2, 1)
    router_a_t = router_a.transpose(0, 2, 1)
    shared = (gain_one, gain_two, qkv_weight, out_weight, router_t)
    adapters = (qkv_a_t, qkv_b, out_a_t, out_b, router_a_t, router_b)
    grid_of = functools.partial(pltpu.PrefetchScalarGridSpec, num_scalar_prefetch=1)
    forward_out = (
        jax.ShapeDtypeStruct((n_images, padded, 3 * width), LOW),
        jax.ShapeDtypeStruct((n_images, padded, width), LOW),
        jax.ShapeDtypeStruct((n_images, padded, width), F32),
        jax.ShapeDtypeStruct((n_images, padded, width), LOW),
        jax.ShapeDtypeStruct((n_images, padded, 2), F32),
        jax.ShapeDtypeStruct((n_images, 2, padded), F32),
    )
    qkv, context, hidden, normed, gates, gate_rows = pl.pallas_call(
        functools.partial(forward_kernel, seq_len),
        out_shape=forward_out,
        grid_spec=grid_of(
            grid=(n_images,),
            in_specs=[per_image(a) for a in (images, picks, pick_rows)]
            + [whole(a) for a in shared]
            + [per_adapter(a) for a in adapters],
            out_specs=[per_image(a) for a in forward_out],
        ),
        name="attend",
        cost_estimate=work_of(20),
    )(adapter_ids, images, picks, pick_rows, *shared, *adapters)

    normed_all = lax.all_gather(normed.reshape(rows, width), "expert")
    gates_all = lax.all_gather(gate_rows.transpose(1, 0, 2).reshape(2, rows), "expert")
    up_a_t = up_a.transpose(0, 1, 3, 2).reshape(local, low_cols, width)
    up_b_flat = up_b.reshape(local, low_cols, ff_width)
    down_a_t = down_a.transpose(0, 1, 3, 2).reshape(local, low_cols, ff_width)
    down_b_flat = down_b.reshape(local, low_cols, width)
    cols = 2 * width + 2 * ff_width
    backs, sums, raw = [], [], []
    for piece in range(PIECES):
        at = piece * here

        def of_expert(array, at=at):
            rank = len(array.shape)
            return pl.BlockSpec(
                (1,) + array.shape[1:], lambda i, s: (i + at,) + (0,) * (rank - 1)
            )

        weights = (up_weight, down_weight, up_a_t, up_b_flat, down_a_t, down_b_flat)
        first = ((piece * groups + lax.axis_index("expert")) * here).astype(jnp.int32)
        gathered = (side_all, gates_all, normed_all, upstream_all)
        after = tuple(raw[-1:])
        n_rows = groups * room
        back, grads = pl.pallas_call(
            functools.partial(expert_kernel, len(after)),
            out_shape=(
                jax.ShapeDtypeStruct((groups, here, room, 2 * width), LOW),
                jax.ShapeDtypeStruct((here, low_cols, cols), LOW),
            ),
            grid_spec=grid_of(
                grid=(here,),
                in_specs=[whole(a) for a in gathered]
                + [of_expert(a) for a in weights]
                + [pl.BlockSpec(memory_space=pl.ANY) for a in after],
                out_specs=[
                    pl.BlockSpec((groups, 1, room, 2 * width), lambda i, s: (0, i, 0, 0)),
                    pl.BlockSpec((1, low_cols, cols), lambda i, s: (i, 0, 0)),
                ],
                scratch_shapes=[
                    pltpu.VMEM((n_rows, width), LOW),
                    pltpu.VMEM((n_rows, width), LOW),
                    pltpu.VMEM((n_rows, low_cols), F32),
                    pltpu.VMEM((n_rows, width), F32),
                    pltpu.VMEM((n_rows, width), F32),
                    pltpu.VMEM((n_rows, low_cols), F32),
                    pltpu.VMEM((n_rows, low_cols), F32),
                    pltpu.VMEM((2, low_cols, n_rows), LOW),
                ],
            ),
            cost_estimate=work_of(28),
        )(first.reshape(1), *gathered, *weights, *after)
        raw.append(back)
        backs.append(lax.all_to_all(back, "expert", split_axis=0, concat_axis=0, tiled=True))
        sums.append(sum_over_copies(grads, piece > 0))
    backs = [back.reshape(groups * here * room, 2 * width) for back in backs]

    grad_cols = 8 * width
    tiles = grad_cols // 128
    out_types = (
        jax.ShapeDtypeStruct((n_images, seq_len, width), LOW),
        jax.ShapeDtypeStruct((n_images, seq_len, width), F32),
        jax.ShapeDtypeStruct((n_adapt, tiles, rank, 128), LOW),
    )
    by_image = (images, upstream, hidden, normed, qkv, context, gates, picks, slot_columns)
    block_out, input_grad, own_grads = pl.pallas_call(
        functools.partial(backward_kernel, seq_len),
        out_shape=out_types,
        grid_spec=grid_of(
            grid=(n_images,),
            in_specs=[per_image(a) for a in by_image]
            + [whole(a) for a in shared]
            + [per_adapter(a) for a in adapters]
            + [whole(a) for a in backs],
            out_specs=[per_image(out_types[0]), per_image(out_types[1]), whole(out_types[2])],
            scratch_shapes=[
                pltpu.VMEM((n_adapt, rank, grad_cols), F32),
                pltpu.VMEM((padded, 3 * width), LOW),
            ],
        ),
        name="attend_back",
        cost_estimate=work_of(40),
    )(adapter_ids, *by_image, *shared, *adapters, *backs)
    own_grads = sum_over_all(own_grads.reshape(-1, 128)).reshape(n_adapt, tiles, rank, 128)

    def own_part(start, length):
        part = own_grads[:, start // 128 : -(-(start + length) // 128)].astype(F32)
        return part.transpose(0, 2, 1, 3).reshape(n_adapt, rank, -1)[:, :, :length]

    grad_qkv_a = own_part(0, width).transpose(0, 2, 1)
    grad_qkv_b = own_part(width, 3 * width)
    grad_out_a = own_part(4 * width, width).transpose(0, 2, 1)
    grad_out_b = own_part(5 * width, width)
    grad_router_a = own_part(6 * width, width).transpose(0, 2, 1)
    grad_router_b = own_part(7 * width, n_experts)

    def expert_part(start, length):
        parts = [total[:, :, start : start + length].astype(F32) for total in sums]
        return jnp.concatenate(parts, axis=0).reshape(local, n_adapt, rank, length)

    grad_up_a = expert_part(0, width).transpose(0, 1, 3, 2)
    grad_up_b = expert_part(width, ff_width)
    grad_down_a = expert_part(width + ff_width, ff_width).transpose(0, 1, 3, 2)
    grad_down_b = expert_part(width + 2 * ff_width, width)
    return (
        block_out,
        input_grad,
        grad_qkv_a,
        grad_qkv_b,
        grad_out_a,
        grad_out_b,
        grad_router_a,
        grad_router_b,
        grad_up_a,
        grad_up_b,
        grad_down_a,
        grad_down_b,
    )


def solution(mesh):
    tokens = P(("dp", "expert"), None, None)
    experts = P("expert", None, None, None)
    weights = P("expert", None, None)
    placed = (
        (tokens, P(("dp", "expert")), tokens, tokens)
        + (P(),) * 5
        + (weights,) * 2
        + (P(),) * 6
        + (experts,) * 4
    )

    return jax.shard_map(
        body,
        mesh=mesh,
        in_specs=placed,
        out_specs=(tokens, tokens) + (P(),) * 6 + (experts,) * 4,
        check_vma=False,
    )
```

```python
import functools

import jax
import jax.numpy as jnp
from jax import lax
from jax.experimental import pallas as pl
from jax.experimental.pallas import tpu as pltpu
from jax.sharding import PartitionSpec as P

HEADS = 8
EPSILON = 1e-06
F32 = jnp.float32
LOW = jnp.bfloat16
PIECES = 2
CHUNK = 512


def nn(left, right):
    return lax.dot_general(left, right, (((1,), (0,)), ((), ())), preferred_element_type=F32)


def nt(left, right):
    return lax.dot_general(left, right, (((1,), (1,)), ((), ())), preferred_element_type=F32)


def tn(left, right):
    return lax.dot_general(left, right, (((0,), (0,)), ((), ())), preferred_element_type=F32)


def normalise(values):
    average = jnp.mean(values, axis=-1, keepdims=True)
    centred = values - average
    spread = jnp.mean(centred * centred, axis=-1, keepdims=True)
    factor = lax.rsqrt(spread + EPSILON)
    return centred * factor, factor


def norm_back(grad, normed, factor, gain):
    scaled = grad * gain
    return factor * (
        scaled
        - jnp.mean(scaled, axis=-1, keepdims=True)
        - normed * jnp.mean(scaled * normed, axis=-1, keepdims=True)
    )


def soften(queries, keys, scale, real):
    scores = nt(queries, keys) * scale
    lanes = lax.broadcasted_iota(jnp.int32, scores.shape, 1)
    scores = jnp.where(lanes < real, scores, -1e30)
    powers = jnp.exp(scores - jnp.max(scores, axis=-1, keepdims=True))
    return powers * (1.0 / jnp.sum(powers, axis=-1, keepdims=True))


def pair_gates(first, second):
    top = jnp.maximum(first, second)
    one, two = jnp.exp(first - top), jnp.exp(second - top)
    total = 1.0 / (one + two)
    return one * total, two * total


def forward_kernel(
    real,
    ids_ref,
    images_ref,
    picks_ref,
    pick_rows_ref,
    gain1_ref,
    gain2_ref,
    wqkv_ref,
    wout_ref,
    wrouter_ref,
    qkv_a_ref,
    qkv_b_ref,
    out_a_ref,
    out_b_ref,
    router_a_ref,
    router_b_ref,
    qkv_ref,
    context_ref,
    hidden_ref,
    normed_ref,
    gates_ref,
    gate_rows_ref,
):
    width = images_ref.shape[2]
    size = width // HEADS
    scale = size ** (-0.5)
    inputs = images_ref[0].astype(F32)
    plain, _ = normalise(inputs)
    normed = (plain * gain1_ref[...]).astype(LOW)
    low_one = nt(normed, qkv_a_ref[0]).astype(LOW)
    qkv_ref[0] = (nn(normed, wqkv_ref[...]) + nn(low_one, qkv_b_ref[0])).astype(LOW)
    parts = []
    for head in range(HEADS):
        at = head * size
        probs = soften(
            qkv_ref[0, :, at : at + size],
            qkv_ref[0, :, width + at : width + at + size],
            scale,
            real,
        ).astype(LOW)
        values = qkv_ref[0, :, 2 * width + at : 2 * width + at + size]
        parts.append(nn(probs, values).astype(LOW))
    context = jnp.concatenate(parts, axis=1)
    context_ref[0] = context
    low_two = nt(context, out_a_ref[0]).astype(LOW)
    hidden = inputs + nn(context, wout_ref[...]) + nn(low_two, out_b_ref[0])
    hidden_ref[0] = hidden
    plain_two, _ = normalise(hidden)
    normed_two = (plain_two * gain2_ref[...]).astype(LOW)
    normed_ref[0] = normed_two
    low_router = nt(normed_two, router_a_ref[0]).astype(LOW)
    logits = nt(normed_two, wrouter_ref[...]) + nn(low_router, router_b_ref[0])
    lanes = lax.broadcasted_iota(jnp.int32, logits.shape, 1)
    chosen = [
        jnp.sum(jnp.where(lanes == picks_ref[0, :, k : k + 1], logits, 0.0), axis=1, keepdims=True)
        for k in range(2)
    ]
    gates_ref[0] = jnp.concatenate(pair_gates(*chosen), axis=1)
    low_rows = nt(router_a_ref[0], normed_two).astype(LOW)
    logit_rows = nt(wrouter_ref[...], normed_two) + tn(router_b_ref[0], low_rows)
    places = lax.broadcasted_iota(jnp.int32, logit_rows.shape, 0)
    chosen_rows = [
        jnp.sum(
            jnp.where(places == pick_rows_ref[0, k : k + 1, :], logit_rows, 0.0),
            axis=0,
            keepdims=True,
        )
        for k in range(2)
    ]
    gate_rows_ref[0] = jnp.concatenate(pair_gates(*chosen_rows), axis=0)


def gelu_pair(values):
    half = 0.5 * (1.0 + lax.erf(values * 0.7071067811865476))
    density = jnp.exp(values * values * -0.5) * 0.3989422804014327
    return values * half, half + values * density


def expert_kernel(n_after, groups, first_ref, marks_ref, gate_rows_ref, *rest):
    token_refs, upstream_refs, rest = rest[:groups], rest[groups : 2 * groups], rest[2 * groups :]
    up_ref, down_ref, up_a_ref, up_b_ref, down_a_ref, down_b_ref = rest[:6]
    rest = rest[6:]
    back_ref, grads_ref, rows_ref, dy_ref, mask_ref = rest[n_after : n_after + 5]
    y_ref, dx_ref, low_ref, low_grad_ref, half_ref = rest[n_after + 5 :]
    _, _, capacity, double = back_ref.shape
    width = double // 2
    ff_width = up_ref.shape[2]
    low_cols = up_a_ref.shape[1]
    rank = 16
    start = (first_ref[0] + pl.program_id(0)) * capacity
    for group in range(groups):
        span = slice(group * capacity, (group + 1) * capacity)
        source = first_ref[1 + group]
        n_tokens = token_refs[group].shape[0]
        slots = lax.broadcasted_iota(jnp.int32, (capacity, n_tokens), 0) + start
        zero = slots == marks_ref[source, 0:1, :]
        one = slots == marks_ref[source, 1:2, :]
        either = jnp.where(zero | one, 1.0, 0.0)
        gate = jnp.sum(
            jnp.where(zero, gate_rows_ref[source, 0:1, :], 0.0)
            + jnp.where(one, gate_rows_ref[source, 1:2, :], 0.0),
            axis=1,
            keepdims=True,
        )
        ids = jnp.sum(
            either * marks_ref[source, 2:3, :].astype(F32), axis=1, keepdims=True
        )
        either = either.astype(LOW)
        rows_ref[span, :] = nn(either, token_refs[group][...]).astype(LOW)
        dy_ref[span, :] = (gate * nn(either, upstream_refs[group][...])).astype(LOW)
        cols = lax.broadcasted_iota(jnp.int32, (capacity, low_cols), 1) // rank
        mask_ref[span, :] = jnp.where(cols.astype(F32) == ids, 1.0, 0.0)
    mask = mask_ref[...]
    up_low = (nt(rows_ref[...], up_a_ref[0]) * mask).astype(LOW)
    down_low_grad = (nt(dy_ref[...], down_b_ref[0]) * mask).astype(LOW)
    half_ref[0] = up_low.T
    half_ref[1] = down_low_grad.T
    y_ref[...] = jnp.zeros_like(y_ref)
    dx_ref[...] = jnp.zeros_like(dx_ref)
    low_ref[...] = jnp.zeros_like(low_ref)
    low_grad_ref[...] = jnp.zeros_like(low_grad_ref)
    up_b_at, down_a_at, down_b_at = width, width + ff_width, width + 2 * ff_width

    def step(number, carry):
        at = pl.multiple_of(number * CHUNK, CHUNK)
        cols = pl.ds(at, CHUNK)
        pre = nn(rows_ref[...], up_ref[0, :, cols]) + nn(up_low, up_b_ref[0, :, cols])
        hidden, slope = gelu_pair(pre)
        hidden = hidden.astype(LOW)
        grad = nt(dy_ref[...], down_ref[0, cols, :]) + nn(down_low_grad, down_a_ref[0, :, cols])
        grad = (grad * slope).astype(LOW)
        y_ref[...] += nn(hidden, down_ref[0, cols, :])
        low_ref[...] += nt(hidden, down_a_ref[0, :, cols])
        dx_ref[...] += nt(grad, up_ref[0, :, cols])
        low_grad_ref[...] += nt(grad, up_b_ref[0, :, cols])
        grads_ref[0, :, pl.ds(pl.multiple_of(up_b_at + at, CHUNK), CHUNK)] = nn(
            half_ref[0], grad
        ).astype(LOW)
        grads_ref[0, :, pl.ds(pl.multiple_of(down_a_at + at, CHUNK), CHUNK)] = nn(
            half_ref[1], hidden
        ).astype(LOW)
        return carry

    lax.fori_loop(0, ff_width // CHUNK, step, 0)
    down_low = (low_ref[...] * mask).astype(LOW)
    up_low_grad = (low_grad_ref[...] * mask).astype(LOW)
    out = (y_ref[...] + nn(down_low, down_b_ref[0])).astype(LOW)
    dx = (dx_ref[...] + nn(up_low_grad, up_a_ref[0])).astype(LOW)
    for group in range(groups):
        span = slice(group * capacity, (group + 1) * capacity)
        source = first_ref[1 + group]
        back_ref[source, 0, :, :width] = out[span]
        back_ref[source, 0, :, width:] = dx[span]
    grads_ref[0, :, 0:width] = tn(up_low_grad, rows_ref[...]).astype(LOW)
    grads_ref[0, :, down_b_at : down_b_at + width] = tn(down_low, dy_ref[...]).astype(LOW)


def backward_kernel(
    real,
    ids_ref,
    images_ref,
    upstream_ref,
    hidden_ref,
    normed_ref,
    qkv_ref,
    context_ref,
    gates_ref,
    picks_ref,
    slots_ref,
    gain1_ref,
    gain2_ref,
    wqkv_ref,
    wout_ref,
    wrouter_ref,
    qkv_a_ref,
    qkv_b_ref,
    out_a_ref,
    out_b_ref,
    router_a_ref,
    router_b_ref,
    *rest,
):
    back_refs = rest[:-5]
    out_ref, input_grad_ref, grads_ref, total_ref, dqkv_ref = rest[-5:]
    image = pl.program_id(0)
    own = ids_ref[image]
    width = images_ref.shape[2]
    size = width // HEADS
    scale = size ** (-0.5)
    n_experts = wrouter_ref.shape[0]

    @pl.when(image == 0)
    def _():
        total_ref[...] = jnp.zeros_like(total_ref)

    rows = images_ref.shape[1]
    pair_zero = pair_one = spread = None
    for number, back_ref in enumerate(back_refs):
        n_slots = back_ref.shape[0]
        slots = lax.broadcasted_iota(jnp.int32, (rows, n_slots), 1) + number * n_slots
        zero = jnp.where(slots == slots_ref[0, :, 0:1], 1.0, 0.0).astype(LOW)
        one = jnp.where(slots == slots_ref[0, :, 1:2], 1.0, 0.0).astype(LOW)
        terms = (
            nn(zero, back_ref[:, :width]),
            nn(one, back_ref[:, :width]),
            nn(zero + one, back_ref[:, width:]),
        )
        if number == 0:
            pair_zero, pair_one, spread = terms
        else:
            pair_zero, pair_one, spread = (
                pair_zero + terms[0],
                pair_one + terms[1],
                spread + terms[2],
            )
    gate_zero, gate_one = gates_ref[0, :, 0:1], gates_ref[0, :, 1:2]
    hidden = hidden_ref[0]
    out = (hidden + (gate_zero * pair_zero + gate_one * pair_one)).astype(LOW)
    out_ref[0] = out[:real]
    upstream = upstream_ref[0].astype(F32)
    grad_zero = jnp.sum(upstream * pair_zero, axis=1, keepdims=True)
    grad_one = jnp.sum(upstream * pair_one, axis=1, keepdims=True)
    centre = gate_zero * grad_zero + gate_one * grad_one
    lanes = lax.broadcasted_iota(jnp.int32, (rows, n_experts), 1)
    logits_grad = (
        jnp.where(lanes == picks_ref[0, :, 0:1], gate_zero * (grad_zero - centre), 0.0)
        + jnp.where(lanes == picks_ref[0, :, 1:2], gate_one * (grad_one - centre), 0.0)
    ).astype(LOW)
    normed_two = normed_ref[0]
    low_rows = nt(router_a_ref[0], normed_two).astype(LOW)
    router_low_grad = nt(logits_grad, router_b_ref[0]).astype(LOW)
    qkv_b_at, out_a_at, out_b_at = width, 4 * width, 5 * width
    router_a_at, router_b_at = 6 * width, 7 * width
    total_ref[own, :, router_b_at : router_b_at + n_experts] += nn(low_rows, logits_grad)
    total_ref[own, :, router_a_at : router_a_at + width] += tn(router_low_grad, normed_two)
    spread = spread + nn(logits_grad, wrouter_ref[...]) + nn(router_low_grad, router_a_ref[0])
    plain_two, factor_two = normalise(hidden)
    hidden_grad = upstream + norm_back(spread, plain_two, factor_two, gain2_ref[...])
    branch = hidden_grad.astype(LOW)
    context = context_ref[0]
    low_two = nt(context, out_a_ref[0]).astype(LOW)
    out_low_grad = nt(branch, out_b_ref[0]).astype(LOW)
    total_ref[own, :, out_b_at : out_b_at + width] += tn(low_two, branch)
    total_ref[own, :, out_a_at : out_a_at + width] += tn(out_low_grad, context)
    context_grad = (nt(branch, wout_ref[...]) + nn(out_low_grad, out_a_ref[0])).astype(LOW)
    for head in range(HEADS):
        at = head * size
        queries = qkv_ref[0, :, at : at + size]
        keys = qkv_ref[0, :, width + at : width + at + size]
        values = qkv_ref[0, :, 2 * width + at : 2 * width + at + size]
        own_grad = context_grad[:, at : at + size]
        probs = soften(queries, keys, scale, real)
        probs_grad = nt(own_grad, values)
        score_grad = (
            probs * (probs_grad - jnp.sum(probs_grad * probs, axis=-1, keepdims=True))
        ).astype(LOW)
        dqkv_ref[:, at : at + size] = (nn(score_grad, keys) * scale).astype(LOW)
        dqkv_ref[:, width + at : width + at + size] = (tn(score_grad, queries) * scale).astype(LOW)
        dqkv_ref[:, 2 * width + at : 2 * width + at + size] = tn(
            probs.astype(LOW), own_grad
        ).astype(LOW)
    plain, factor = normalise(images_ref[0].astype(F32))
    normed = (plain * gain1_ref[...]).astype(LOW)
    low_one = nt(normed, qkv_a_ref[0]).astype(LOW)
    dqkv = dqkv_ref[...]
    qkv_low_grad = nt(dqkv, qkv_b_ref[0]).astype(LOW)
    total_ref[own, :, qkv_b_at : qkv_b_at + 3 * width] += tn(low_one, dqkv)
    total_ref[own, :, 0:width] += tn(qkv_low_grad, normed)
    normed_grad = nt(dqkv, wqkv_ref[...]) + nn(qkv_low_grad, qkv_a_ref[0])
    input_grad = hidden_grad + norm_back(normed_grad, plain, factor, gain1_ref[...])
    input_grad_ref[0] = input_grad[:real]

    @pl.when(image == pl.num_programs(0) - 1)
    def _():
        for tile in range(total_ref.shape[2] // 128):
            grads_ref[:, tile] = total_ref[:, :, tile * 128 : tile * 128 + 128].astype(LOW)


def gather_blocks(block, axis):
    count = lax.axis_size(axis)
    far = count // 2
    blocks = [block]
    for hop in range(1, far):
        pairs = [(i, (i // 2 + hop) % far * 2 + i % 2) for i in range(count)]
        blocks.append(lax.ppermute(block, axis, pairs))
    pairs = [(i, i ^ 1) for i in range(count)]
    return blocks + [lax.ppermute(part, axis, pairs) for part in blocks]


def block_sources(axis):
    count = lax.axis_size(axis)
    far = count // 2
    place = lax.axis_index(axis)
    hops = jnp.arange(far, dtype=jnp.int32)
    sources = (place // 2 - hops + far) % far * 2
    return jnp.concatenate([sources + place % 2, sources + 1 - place % 2])


def exchange(values, axis):
    count = lax.axis_size(axis)
    parts = values.reshape(count, -1, values.shape[-1])
    return lax.all_to_all(parts, axis, split_axis=0, concat_axis=0, tiled=True)


def exchange_sum(values, axis):
    return jnp.sum(exchange(values, axis).astype(F32), axis=0).astype(LOW)


def exchange_gather(values, axis):
    count = lax.axis_size(axis)
    copies = jnp.broadcast_to(values[None], (count,) + values.shape)
    copies = lax.all_to_all(copies, axis, split_axis=0, concat_axis=0, tiled=True)
    return copies.reshape(count * values.shape[0], values.shape[1])


def direct_parts(values, axis):
    count = lax.axis_size(axis)
    place = lax.axis_index(axis)
    parts = values.reshape(count, -1, values.shape[-1])
    found = [lax.dynamic_index_in_dim(parts, place, 0, keepdims=False)]
    for hop in range(1, count):
        pairs = [(i, (i + hop) % count) for i in range(count)]
        part = lax.dynamic_index_in_dim(parts, (place + hop) % count, 0, keepdims=False)
        found.append(lax.ppermute(part, axis, pairs))
    return found


def sum_kernel(count, *refs):
    total = refs[0][...].astype(F32)
    for number in range(1, count):
        total = total + refs[number][...].astype(F32)
    refs[-1][...] = total.astype(LOW)


def sum_after(parts, after):
    rows, cols = parts[0].shape
    block = pl.BlockSpec((rows, 512), lambda i: (0, i))
    return pl.pallas_call(
        functools.partial(sum_kernel, len(parts)),
        out_shape=jax.ShapeDtypeStruct((rows, cols), LOW),
        grid=(cols // 512,),
        in_specs=[block] * len(parts) + [pl.BlockSpec(memory_space=pl.ANY)],
        out_specs=block,
        name="add_parts",
    )(*parts, after)


def work_of(microseconds):
    return pl.CostEstimate(flops=microseconds * 10**9, bytes_accessed=10**6, transcendentals=0)


def whole(array):
    rank = len(array.shape)
    return pl.BlockSpec(array.shape, lambda i, s: (0,) * rank)


def per_image(array):
    rank = len(array.shape)
    return pl.BlockSpec((1,) + array.shape[1:], lambda i, s: (i,) + (0,) * (rank - 1))


def per_adapter(array):
    rank = len(array.shape)
    return pl.BlockSpec((1,) + array.shape[1:], lambda i, s: (s[i],) + (0,) * (rank - 1))


def body(
    images,
    adapter_ids,
    expert_ids,
    cotangent,
    ln_gain1,
    ln_gain2,
    qkv_weight,
    out_weight,
    router_weight,
    up_weight,
    down_weight,
    qkv_a,
    qkv_b,
    out_a,
    out_b,
    router_a,
    router_b,
    up_a,
    up_b,
    down_a,
    down_b,
):
    n_images, seq_len, width = images.shape
    tokens = n_images * seq_len
    padded = -(-seq_len // 16) * 16
    rows = n_images * padded
    n_adapt, _, rank = qkv_a.shape
    low_cols = n_adapt * rank
    n_experts = router_weight.shape[1]
    local = up_weight.shape[0]
    ff_width = up_weight.shape[2]
    groups = lax.axis_size("expert")
    capacity = max(2, tokens * 2 * 5 // (4 * n_experts))
    room = -(-capacity // 16) * 16
    here = local // PIECES

    fill = ((0, 0), (0, padded - seq_len), (0, 0))
    images = jnp.pad(images, fill)
    upstream = jnp.pad(cotangent, fill)
    picks = jnp.pad(expert_ids, fill, constant_values=-1)
    pick_rows = picks.transpose(0, 2, 1)
    flat = pick_rows.transpose(1, 0, 2).reshape(2, rows)
    marks = flat[:, None, :] == jnp.arange(n_experts, dtype=jnp.int32)[None, :, None]
    order = jnp.arange(rows, dtype=jnp.int32)
    earlier = (order[:, None] < order[None, :]).astype(LOW)
    before = jnp.dot(
        marks.reshape(2 * n_experts, rows).astype(LOW), earlier, preferred_element_type=F32
    ).reshape(2, n_experts, rows)
    totals = jnp.sum(marks[0].astype(F32), axis=1)
    offset = jnp.stack([jnp.zeros_like(totals), totals])
    places = jnp.sum(
        jnp.where(marks, before + offset[:, :, None], 0.0), axis=1
    ).astype(jnp.int32)
    group_of, inner = flat // local, flat % local
    ranked = ((inner // here) * groups + group_of) * here + inner % here
    kept = (flat >= 0) & (places < capacity)
    slots = jnp.where(kept, ranked * room + places, -1)
    token_ids = jnp.broadcast_to(adapter_ids[:, None], (n_images, padded)).reshape(1, rows)
    slot_columns = slots.reshape(2, n_images, padded).transpose(1, 2, 0)
    side = jnp.concatenate([slots, token_ids], axis=0)
    side_all = lax.all_gather(side, "expert")
    upstream_all = gather_blocks(upstream.reshape(rows, width), "expert")

    gain_one = ln_gain1.astype(F32).reshape(1, width)
    gain_two = ln_gain2.astype(F32).reshape(1, width)
    router_t = router_weight.T
    qkv_a_t = qkv_a.transpose(0, 2, 1)
    out_a_t = out_a.transpose(0, 2, 1)
    router_a_t = router_a.transpose(0, 2, 1)
    shared = (gain_one, gain_two, qkv_weight, out_weight, router_t)
    adapters = (qkv_a_t, qkv_b, out_a_t, out_b, router_a_t, router_b)
    grid_of = functools.partial(pltpu.PrefetchScalarGridSpec, num_scalar_prefetch=1)
    forward_out = (
        jax.ShapeDtypeStruct((n_images, padded, 3 * width), LOW),
        jax.ShapeDtypeStruct((n_images, padded, width), LOW),
        jax.ShapeDtypeStruct((n_images, padded, width), F32),
        jax.ShapeDtypeStruct((n_images, padded, width), LOW),
        jax.ShapeDtypeStruct((n_images, padded, 2), F32),
        jax.ShapeDtypeStruct((n_images, 2, padded), F32),
    )
    qkv, context, hidden, normed, gates, gate_rows = pl.pallas_call(
        functools.partial(forward_kernel, seq_len),
        out_shape=forward_out,
        grid_spec=grid_of(
            grid=(n_images,),
            in_specs=[per_image(a) for a in (images, picks, pick_rows)]
            + [whole(a) for a in shared]
            + [per_adapter(a) for a in adapters],
            out_specs=[per_image(a) for a in forward_out],
        ),
        name="attend",
        cost_estimate=work_of(20),
    )(adapter_ids, images, picks, pick_rows, *shared, *adapters)

    normed_all = gather_blocks(normed.reshape(rows, width), "expert")
    sources = block_sources("expert")
    gates_all = lax.all_gather(gate_rows.transpose(1, 0, 2).reshape(2, rows), "expert")
    up_a_t = up_a.transpose(0, 1, 3, 2).reshape(local, low_cols, width)
    up_b_flat = up_b.reshape(local, low_cols, ff_width)
    down_a_t = down_a.transpose(0, 1, 3, 2).reshape(local, low_cols, ff_width)
    down_b_flat = down_b.reshape(local, low_cols, width)
    cols = 2 * width + 2 * ff_width
    backs, sums, raw = [], [], []
    for piece in range(PIECES):
        at = piece * here

        def of_expert(array, at=at):
            rank = len(array.shape)
            return pl.BlockSpec(
                (1,) + array.shape[1:], lambda i, s: (i + at,) + (0,) * (rank - 1)
            )

        weights = (up_weight, down_weight, up_a_t, up_b_flat, down_a_t, down_b_flat)
        first = ((piece * groups + lax.axis_index("expert")) * here).astype(jnp.int32)
        gathered = (side_all, gates_all, *normed_all, *upstream_all)
        after = tuple(raw[-1:])
        n_rows = groups * room
        back, grads = pl.pallas_call(
            functools.partial(expert_kernel, len(after), groups),
            out_shape=(
                jax.ShapeDtypeStruct((groups, here, room, 2 * width), LOW),
                jax.ShapeDtypeStruct((here, low_cols, cols), LOW),
            ),
            grid_spec=grid_of(
                grid=(here,),
                in_specs=[whole(a) for a in gathered]
                + [of_expert(a) for a in weights]
                + [pl.BlockSpec(memory_space=pl.ANY) for a in after],
                out_specs=[
                    pl.BlockSpec((groups, 1, room, 2 * width), lambda i, s: (0, i, 0, 0)),
                    pl.BlockSpec((1, low_cols, cols), lambda i, s: (i, 0, 0)),
                ],
                scratch_shapes=[
                    pltpu.VMEM((n_rows, width), LOW),
                    pltpu.VMEM((n_rows, width), LOW),
                    pltpu.VMEM((n_rows, low_cols), F32),
                    pltpu.VMEM((n_rows, width), F32),
                    pltpu.VMEM((n_rows, width), F32),
                    pltpu.VMEM((n_rows, low_cols), F32),
                    pltpu.VMEM((n_rows, low_cols), F32),
                    pltpu.VMEM((2, low_cols, n_rows), LOW),
                ],
            ),
            cost_estimate=work_of(28),
        )(jnp.concatenate([first.reshape(1), sources]), *gathered, *weights, *after)
        raw.append(back)
        backs.append(lax.all_to_all(back, "expert", split_axis=0, concat_axis=0, tiled=True))
        sums.append(lax.psum(grads, "dp") if piece == 0 else direct_parts(grads, "dp"))
    backs = [back.reshape(groups * here * room, 2 * width) for back in backs]

    grad_cols = 8 * width
    tiles = grad_cols // 128
    out_types = (
        jax.ShapeDtypeStruct((n_images, seq_len, width), LOW),
        jax.ShapeDtypeStruct((n_images, seq_len, width), F32),
        jax.ShapeDtypeStruct((n_adapt, tiles, rank, 128), LOW),
    )
    by_image = (images, upstream, hidden, normed, qkv, context, gates, picks, slot_columns)
    block_out, input_grad, own_grads = pl.pallas_call(
        functools.partial(backward_kernel, seq_len),
        out_shape=out_types,
        grid_spec=grid_of(
            grid=(n_images,),
            in_specs=[per_image(a) for a in by_image]
            + [whole(a) for a in shared]
            + [per_adapter(a) for a in adapters]
            + [whole(a) for a in backs],
            out_specs=[per_image(out_types[0]), per_image(out_types[1]), whole(out_types[2])],
            scratch_shapes=[
                pltpu.VMEM((n_adapt, rank, grad_cols), F32),
                pltpu.VMEM((padded, 3 * width), LOW),
            ],
        ),
        name="attend_back",
        cost_estimate=work_of(40),
    )(adapter_ids, *by_image, *shared, *adapters, *backs)
    part = exchange_sum(own_grads.reshape(-1, 128), "expert")
    part = exchange_sum(part, "dp")
    last = lax.all_gather(sum_after(sums[1], part), "dp", axis=0, tiled=True)
    sums[1] = last.reshape(sums[0].shape)
    part = exchange_gather(part, "dp")
    part = exchange_gather(part, "expert")
    own_grads = part.reshape(n_adapt, tiles, rank, 128)

    def own_part(start, length):
        part = own_grads[:, start // 128 : -(-(start + length) // 128)].astype(F32)
        return part.transpose(0, 2, 1, 3).reshape(n_adapt, rank, -1)[:, :, :length]

    grad_qkv_a = own_part(0, width).transpose(0, 2, 1)
    grad_qkv_b = own_part(width, 3 * width)
    grad_out_a = own_part(4 * width, width).transpose(0, 2, 1)
    grad_out_b = own_part(5 * width, width)
    grad_router_a = own_part(6 * width, width).transpose(0, 2, 1)
    grad_router_b = own_part(7 * width, n_experts)

    def expert_part(start, length):
        parts = [total[:, :, start : start + length].astype(F32) for total in sums]
        return jnp.concatenate(parts, axis=0).reshape(local, n_adapt, rank, length)

    grad_up_a = expert_part(0, width).transpose(0, 1, 3, 2)
    grad_up_b = expert_part(width, ff_width)
    grad_down_a = expert_part(width + ff_width, ff_width).transpose(0, 1, 3, 2)
    grad_down_b = expert_part(width + 2 * ff_width, width)
    return (
        block_out,
        input_grad,
        grad_qkv_a,
        grad_qkv_b,
        grad_out_a,
        grad_out_b,
        grad_router_a,
        grad_router_b,
        grad_up_a,
        grad_up_b,
        grad_down_a,
        grad_down_b,
    )


def solution(mesh):
    tokens = P(("dp", "expert"), None, None)
    experts = P("expert", None, None, None)
    weights = P("expert", None, None)
    placed = (
        (tokens, P(("dp", "expert")), tokens, tokens)
        + (P(),) * 5
        + (weights,) * 2
        + (P(),) * 6
        + (experts,) * 4
    )

    return jax.shard_map(
        body,
        mesh=mesh,
        in_specs=placed,
        out_specs=(tokens, tokens) + (P(),) * 6 + (experts,) * 4,
        check_vma=False,
    )
```

```python
import functools

import jax
import jax.numpy as jnp
from jax import lax
from jax.experimental import pallas as pl
from jax.experimental.pallas import tpu as pltpu
from jax.sharding import PartitionSpec as P

HEADS = 8
EPSILON = 1e-06
F32 = jnp.float32
LOW = jnp.bfloat16
CHUNK = 512


def nn(left, right):
    return lax.dot_general(left, right, (((1,), (0,)), ((), ())), preferred_element_type=F32)


def nt(left, right):
    return lax.dot_general(left, right, (((1,), (1,)), ((), ())), preferred_element_type=F32)


def tn(left, right):
    return lax.dot_general(left, right, (((0,), (0,)), ((), ())), preferred_element_type=F32)


def normalise(values):
    average = jnp.mean(values, axis=-1, keepdims=True)
    centred = values - average
    spread = jnp.mean(centred * centred, axis=-1, keepdims=True)
    factor = lax.rsqrt(spread + EPSILON)
    return centred * factor, factor


def norm_back(grad, normed, factor, gain):
    scaled = grad * gain
    return factor * (
        scaled
        - jnp.mean(scaled, axis=-1, keepdims=True)
        - normed * jnp.mean(scaled * normed, axis=-1, keepdims=True)
    )


def soften(queries, keys, scale, real):
    scores = nt(queries, keys) * scale
    lanes = lax.broadcasted_iota(jnp.int32, scores.shape, 1)
    scores = jnp.where(lanes < real, scores, -1e30)
    powers = jnp.exp(scores - jnp.max(scores, axis=-1, keepdims=True))
    return powers * (1.0 / jnp.sum(powers, axis=-1, keepdims=True))


def pair_gates(first, second):
    top = jnp.maximum(first, second)
    one, two = jnp.exp(first - top), jnp.exp(second - top)
    total = 1.0 / (one + two)
    return one * total, two * total


def forward_kernel(
    real,
    ids_ref,
    images_ref,
    picks_ref,
    pick_rows_ref,
    gain1_ref,
    gain2_ref,
    wqkv_ref,
    wout_ref,
    wrouter_ref,
    qkv_a_ref,
    qkv_b_ref,
    out_a_ref,
    out_b_ref,
    router_a_ref,
    router_b_ref,
    qkv_ref,
    context_ref,
    hidden_ref,
    normed_ref,
    gates_ref,
    gate_rows_ref,
):
    width = images_ref.shape[2]
    size = width // HEADS
    scale = size ** (-0.5)
    inputs = images_ref[0].astype(F32)
    plain, _ = normalise(inputs)
    normed = (plain * gain1_ref[...]).astype(LOW)
    low_one = nt(normed, qkv_a_ref[0]).astype(LOW)
    qkv_ref[0] = (nn(normed, wqkv_ref[...]) + nn(low_one, qkv_b_ref[0])).astype(LOW)
    parts = []
    for head in range(HEADS):
        at = head * size
        probs = soften(
            qkv_ref[0, :, at : at + size],
            qkv_ref[0, :, width + at : width + at + size],
            scale,
            real,
        ).astype(LOW)
        values = qkv_ref[0, :, 2 * width + at : 2 * width + at + size]
        parts.append(nn(probs, values).astype(LOW))
    context = jnp.concatenate(parts, axis=1)
    context_ref[0] = context
    low_two = nt(context, out_a_ref[0]).astype(LOW)
    hidden = inputs + nn(context, wout_ref[...]) + nn(low_two, out_b_ref[0])
    hidden_ref[0] = hidden
    plain_two, _ = normalise(hidden)
    normed_two = (plain_two * gain2_ref[...]).astype(LOW)
    normed_ref[0] = normed_two
    low_router = nt(normed_two, router_a_ref[0]).astype(LOW)
    logits = nt(normed_two, wrouter_ref[...]) + nn(low_router, router_b_ref[0])
    lanes = lax.broadcasted_iota(jnp.int32, logits.shape, 1)
    chosen = [
        jnp.sum(jnp.where(lanes == picks_ref[0, :, k : k + 1], logits, 0.0), axis=1, keepdims=True)
        for k in range(2)
    ]
    gates_ref[0] = jnp.concatenate(pair_gates(*chosen), axis=1)
    low_rows = nt(router_a_ref[0], normed_two).astype(LOW)
    logit_rows = nt(wrouter_ref[...], normed_two) + tn(router_b_ref[0], low_rows)
    places = lax.broadcasted_iota(jnp.int32, logit_rows.shape, 0)
    chosen_rows = [
        jnp.sum(
            jnp.where(places == pick_rows_ref[0, k : k + 1, :], logit_rows, 0.0),
            axis=0,
            keepdims=True,
        )
        for k in range(2)
    ]
    gate_rows_ref[0] = jnp.concatenate(pair_gates(*chosen_rows), axis=0)


def gelu_pair(values):
    half = 0.5 * (1.0 + lax.erf(values * 0.7071067811865476))
    density = jnp.exp(values * values * -0.5) * 0.3989422804014327
    return values * half, half + values * density


def expert_kernel(n_after, groups, first_ref, *rest):
    mark_refs, gate_refs = rest[:groups], rest[groups : 2 * groups]
    token_refs, upstream_refs = rest[2 * groups : 3 * groups], rest[3 * groups : 4 * groups]
    rest = rest[4 * groups :]
    up_ref, down_ref, up_a_ref, up_b_ref, down_a_ref, down_b_ref = rest[:6]
    rest = rest[6:]
    back_ref, grads_ref, rows_ref, dy_ref, mask_ref = rest[n_after : n_after + 5]
    y_ref, dx_ref, low_ref, low_grad_ref, half_ref = rest[n_after + 5 :]
    _, _, capacity, double = back_ref.shape
    width = double // 2
    ff_width = up_ref.shape[2]
    low_cols = up_a_ref.shape[1]
    rank = 16
    start = (first_ref[0] + pl.program_id(0)) * capacity
    for group in range(groups):
        span = slice(group * capacity, (group + 1) * capacity)
        marks_ref, gate_rows_ref = mark_refs[group], gate_refs[group]
        n_tokens = token_refs[group].shape[0]
        slots = lax.broadcasted_iota(jnp.int32, (capacity, n_tokens), 0) + start
        zero = slots == marks_ref[0:1, :]
        one = slots == marks_ref[1:2, :]
        either = jnp.where(zero | one, 1.0, 0.0)
        gate = jnp.sum(
            jnp.where(zero, gate_rows_ref[0:1, :], 0.0)
            + jnp.where(one, gate_rows_ref[1:2, :], 0.0),
            axis=1,
            keepdims=True,
        )
        ids = jnp.sum(
            either * marks_ref[2:3, :].astype(F32), axis=1, keepdims=True
        )
        either = either.astype(LOW)
        rows_ref[span, :] = nn(either, token_refs[group][...]).astype(LOW)
        dy_ref[span, :] = (gate * nn(either, upstream_refs[group][...])).astype(LOW)
        cols = lax.broadcasted_iota(jnp.int32, (capacity, low_cols), 1) // rank
        mask_ref[span, :] = jnp.where(cols.astype(F32) == ids, 1.0, 0.0)
    mask = mask_ref[...]
    up_low = (nt(rows_ref[...], up_a_ref[0]) * mask).astype(LOW)
    down_low_grad = (nt(dy_ref[...], down_b_ref[0]) * mask).astype(LOW)
    half_ref[0] = up_low.T
    half_ref[1] = down_low_grad.T
    y_ref[...] = jnp.zeros_like(y_ref)
    dx_ref[...] = jnp.zeros_like(dx_ref)
    low_ref[...] = jnp.zeros_like(low_ref)
    low_grad_ref[...] = jnp.zeros_like(low_grad_ref)
    up_b_at, down_a_at, down_b_at = width, width + ff_width, width + 2 * ff_width

    def step(number, carry):
        at = pl.multiple_of(number * CHUNK, CHUNK)
        cols = pl.ds(at, CHUNK)
        pre = nn(rows_ref[...], up_ref[0, :, cols]) + nn(up_low, up_b_ref[0, :, cols])
        hidden, slope = gelu_pair(pre)
        hidden = hidden.astype(LOW)
        grad = nt(dy_ref[...], down_ref[0, cols, :]) + nn(down_low_grad, down_a_ref[0, :, cols])
        grad = (grad * slope).astype(LOW)
        y_ref[...] += nn(hidden, down_ref[0, cols, :])
        low_ref[...] += nt(hidden, down_a_ref[0, :, cols])
        dx_ref[...] += nt(grad, up_ref[0, :, cols])
        low_grad_ref[...] += nt(grad, up_b_ref[0, :, cols])
        grads_ref[0, :, pl.ds(pl.multiple_of(up_b_at + at, CHUNK), CHUNK)] = nn(
            half_ref[0], grad
        ).astype(LOW)
        grads_ref[0, :, pl.ds(pl.multiple_of(down_a_at + at, CHUNK), CHUNK)] = nn(
            half_ref[1], hidden
        ).astype(LOW)
        return carry

    lax.fori_loop(0, ff_width // CHUNK, step, 0)
    down_low = (low_ref[...] * mask).astype(LOW)
    up_low_grad = (low_grad_ref[...] * mask).astype(LOW)
    out = (y_ref[...] + nn(down_low, down_b_ref[0])).astype(LOW)
    dx = (dx_ref[...] + nn(up_low_grad, up_a_ref[0])).astype(LOW)
    for group in range(groups):
        span = slice(group * capacity, (group + 1) * capacity)
        source = first_ref[1 + group]
        back_ref[source, 0, :, :width] = out[span]
        back_ref[source, 0, :, width:] = dx[span]
    grads_ref[0, :, 0:width] = tn(up_low_grad, rows_ref[...]).astype(LOW)
    grads_ref[0, :, down_b_at : down_b_at + width] = tn(down_low, dy_ref[...]).astype(LOW)


def backward_kernel(
    real,
    ids_ref,
    images_ref,
    upstream_ref,
    hidden_ref,
    normed_ref,
    qkv_ref,
    context_ref,
    gates_ref,
    picks_ref,
    slots_ref,
    gain1_ref,
    gain2_ref,
    wqkv_ref,
    wout_ref,
    wrouter_ref,
    qkv_a_ref,
    qkv_b_ref,
    out_a_ref,
    out_b_ref,
    router_a_ref,
    router_b_ref,
    *rest,
):
    back_refs = rest[:-5]
    out_ref, input_grad_ref, grads_ref, total_ref, dqkv_ref = rest[-5:]
    image = pl.program_id(0)
    own = ids_ref[image]
    width = images_ref.shape[2]
    size = width // HEADS
    scale = size ** (-0.5)
    n_experts = wrouter_ref.shape[0]

    @pl.when(image == 0)
    def _():
        total_ref[...] = jnp.zeros_like(total_ref)

    rows = images_ref.shape[1]
    pair_zero = pair_one = spread = None
    offset = 0
    for number, back_ref in enumerate(back_refs):
        n_slots = back_ref.shape[0]
        slots = lax.broadcasted_iota(jnp.int32, (rows, n_slots), 1) + offset
        offset += n_slots
        zero = jnp.where(slots == slots_ref[0, :, 0:1], 1.0, 0.0).astype(LOW)
        one = jnp.where(slots == slots_ref[0, :, 1:2], 1.0, 0.0).astype(LOW)
        terms = (
            nn(zero, back_ref[:, :width]),
            nn(one, back_ref[:, :width]),
            nn(zero + one, back_ref[:, width:]),
        )
        if number == 0:
            pair_zero, pair_one, spread = terms
        else:
            pair_zero, pair_one, spread = (
                pair_zero + terms[0],
                pair_one + terms[1],
                spread + terms[2],
            )
    gate_zero, gate_one = gates_ref[0, :, 0:1], gates_ref[0, :, 1:2]
    hidden = hidden_ref[0]
    out = (hidden + (gate_zero * pair_zero + gate_one * pair_one)).astype(LOW)
    out_ref[0] = out[:real]
    upstream = upstream_ref[0].astype(F32)
    grad_zero = jnp.sum(upstream * pair_zero, axis=1, keepdims=True)
    grad_one = jnp.sum(upstream * pair_one, axis=1, keepdims=True)
    centre = gate_zero * grad_zero + gate_one * grad_one
    lanes = lax.broadcasted_iota(jnp.int32, (rows, n_experts), 1)
    logits_grad = (
        jnp.where(lanes == picks_ref[0, :, 0:1], gate_zero * (grad_zero - centre), 0.0)
        + jnp.where(lanes == picks_ref[0, :, 1:2], gate_one * (grad_one - centre), 0.0)
    ).astype(LOW)
    normed_two = normed_ref[0]
    low_rows = nt(router_a_ref[0], normed_two).astype(LOW)
    router_low_grad = nt(logits_grad, router_b_ref[0]).astype(LOW)
    qkv_b_at, out_a_at, out_b_at = width, 4 * width, 5 * width
    router_a_at, router_b_at = 6 * width, 7 * width
    total_ref[own, :, router_b_at : router_b_at + n_experts] += nn(low_rows, logits_grad)
    total_ref[own, :, router_a_at : router_a_at + width] += tn(router_low_grad, normed_two)
    spread = spread + nn(logits_grad, wrouter_ref[...]) + nn(router_low_grad, router_a_ref[0])
    plain_two, factor_two = normalise(hidden)
    hidden_grad = upstream + norm_back(spread, plain_two, factor_two, gain2_ref[...])
    branch = hidden_grad.astype(LOW)
    context = context_ref[0]
    low_two = nt(context, out_a_ref[0]).astype(LOW)
    out_low_grad = nt(branch, out_b_ref[0]).astype(LOW)
    total_ref[own, :, out_b_at : out_b_at + width] += tn(low_two, branch)
    total_ref[own, :, out_a_at : out_a_at + width] += tn(out_low_grad, context)
    context_grad = (nt(branch, wout_ref[...]) + nn(out_low_grad, out_a_ref[0])).astype(LOW)
    for head in range(HEADS):
        at = head * size
        queries = qkv_ref[0, :, at : at + size]
        keys = qkv_ref[0, :, width + at : width + at + size]
        values = qkv_ref[0, :, 2 * width + at : 2 * width + at + size]
        own_grad = context_grad[:, at : at + size]
        probs = soften(queries, keys, scale, real)
        probs_grad = nt(own_grad, values)
        score_grad = (
            probs * (probs_grad - jnp.sum(probs_grad * probs, axis=-1, keepdims=True))
        ).astype(LOW)
        dqkv_ref[:, at : at + size] = (nn(score_grad, keys) * scale).astype(LOW)
        dqkv_ref[:, width + at : width + at + size] = (tn(score_grad, queries) * scale).astype(LOW)
        dqkv_ref[:, 2 * width + at : 2 * width + at + size] = tn(
            probs.astype(LOW), own_grad
        ).astype(LOW)
    plain, factor = normalise(images_ref[0].astype(F32))
    normed = (plain * gain1_ref[...]).astype(LOW)
    low_one = nt(normed, qkv_a_ref[0]).astype(LOW)
    dqkv = dqkv_ref[...]
    qkv_low_grad = nt(dqkv, qkv_b_ref[0]).astype(LOW)
    total_ref[own, :, qkv_b_at : qkv_b_at + 3 * width] += tn(low_one, dqkv)
    total_ref[own, :, 0:width] += tn(qkv_low_grad, normed)
    normed_grad = nt(dqkv, wqkv_ref[...]) + nn(qkv_low_grad, qkv_a_ref[0])
    input_grad = hidden_grad + norm_back(normed_grad, plain, factor, gain1_ref[...])
    input_grad_ref[0] = input_grad[:real]

    @pl.when(image == pl.num_programs(0) - 1)
    def _():
        for tile in range(total_ref.shape[2] // 128):
            grads_ref[:, tile] = total_ref[:, :, tile * 128 : tile * 128 + 128].astype(LOW)


def gather_blocks(block, axis):
    count = lax.axis_size(axis)
    far = count // 2
    blocks = [block]
    for hop in range(1, far):
        pairs = [(i, (i // 2 + hop) % far * 2 + i % 2) for i in range(count)]
        blocks.append(lax.ppermute(block, axis, pairs))
    pairs = [(i, i ^ 1) for i in range(count)]
    return blocks + [lax.ppermute(part, axis, pairs) for part in blocks]


def block_sources(axis):
    count = lax.axis_size(axis)
    far = count // 2
    place = lax.axis_index(axis)
    hops = jnp.arange(far, dtype=jnp.int32)
    sources = (place // 2 - hops + far) % far * 2
    return jnp.concatenate([sources + place % 2, sources + 1 - place % 2])


def exchange(values, axis):
    count = lax.axis_size(axis)
    parts = values.reshape(count, -1, values.shape[-1])
    return lax.all_to_all(parts, axis, split_axis=0, concat_axis=0, tiled=True)


def exchange_sum(values, axis):
    return jnp.sum(exchange(values, axis).astype(F32), axis=0).astype(LOW)


def exchange_gather(values, axis):
    count = lax.axis_size(axis)
    copies = jnp.broadcast_to(values[None], (count,) + values.shape)
    copies = lax.all_to_all(copies, axis, split_axis=0, concat_axis=0, tiled=True)
    return copies.reshape(count * values.shape[0], values.shape[1])


def direct_parts(values, axis):
    count = lax.axis_size(axis)
    place = lax.axis_index(axis)
    parts = values.reshape(count, -1, values.shape[-1])
    found = [lax.dynamic_index_in_dim(parts, place, 0, keepdims=False)]
    for hop in range(1, count):
        pairs = [(i, (i + hop) % count) for i in range(count)]
        part = lax.dynamic_index_in_dim(parts, (place + hop) % count, 0, keepdims=False)
        found.append(lax.ppermute(part, axis, pairs))
    return found


def direct_gather(part, axis):
    count = lax.axis_size(axis)
    place = lax.axis_index(axis)
    whole_sum = jnp.zeros((count,) + part.shape, part.dtype)
    found = [part]
    for hop in range(1, count):
        pairs = [(i, (i + hop) % count) for i in range(count)]
        found.append(lax.ppermute(part, axis, pairs))
    for hop, block in enumerate(found):
        spot = (place - hop + count) % count
        whole_sum = lax.dynamic_update_index_in_dim(whole_sum, block, spot, 0)
    return whole_sum.reshape(-1, part.shape[-1])


def sum_kernel(count, *refs):
    total = refs[0][...].astype(F32)
    for number in range(1, count):
        total = total + refs[number][...].astype(F32)
    refs[-1][...] = total.astype(LOW)


def sum_after(parts, after):
    rows, cols = parts[0].shape
    block = pl.BlockSpec((rows, 512), lambda i: (0, i))
    return pl.pallas_call(
        functools.partial(sum_kernel, len(parts)),
        out_shape=jax.ShapeDtypeStruct((rows, cols), LOW),
        grid=(cols // 512,),
        in_specs=[block] * len(parts) + [pl.BlockSpec(memory_space=pl.ANY)],
        out_specs=block,
        name="add_parts",
    )(*parts, after)


def work_of(microseconds):
    return pl.CostEstimate(flops=microseconds * 10**9, bytes_accessed=10**6, transcendentals=0)


def whole(array):
    rank = len(array.shape)
    return pl.BlockSpec(array.shape, lambda i, s: (0,) * rank)


def per_image(array):
    rank = len(array.shape)
    return pl.BlockSpec((1,) + array.shape[1:], lambda i, s: (i,) + (0,) * (rank - 1))


def per_adapter(array):
    rank = len(array.shape)
    return pl.BlockSpec((1,) + array.shape[1:], lambda i, s: (s[i],) + (0,) * (rank - 1))


def body(
    images,
    adapter_ids,
    expert_ids,
    cotangent,
    ln_gain1,
    ln_gain2,
    qkv_weight,
    out_weight,
    router_weight,
    up_weight,
    down_weight,
    qkv_a,
    qkv_b,
    out_a,
    out_b,
    router_a,
    router_b,
    up_a,
    up_b,
    down_a,
    down_b,
):
    n_images, seq_len, width = images.shape
    tokens = n_images * seq_len
    padded = -(-seq_len // 16) * 16
    rows = n_images * padded
    n_adapt, _, rank = qkv_a.shape
    low_cols = n_adapt * rank
    n_experts = router_weight.shape[1]
    local = up_weight.shape[0]
    ff_width = up_weight.shape[2]
    groups = lax.axis_size("expert")
    capacity = max(2, tokens * 2 * 5 // (4 * n_experts))
    room = -(-capacity // 16) * 16
    sizes = (local - 2 * (local // 4), local // 4, local // 4)
    starts = (0, sizes[0], sizes[0] + sizes[1])

    fill = ((0, 0), (0, padded - seq_len), (0, 0))
    images = jnp.pad(images, fill)
    upstream = jnp.pad(cotangent, fill)
    picks = jnp.pad(expert_ids, fill, constant_values=-1)
    pick_rows = picks.transpose(0, 2, 1)
    flat = pick_rows.transpose(1, 0, 2).reshape(2, rows)
    marks = flat[:, None, :] == jnp.arange(n_experts, dtype=jnp.int32)[None, :, None]
    order = jnp.arange(rows, dtype=jnp.int32)
    earlier = (order[:, None] < order[None, :]).astype(LOW)
    before = jnp.dot(
        marks.reshape(2 * n_experts, rows).astype(LOW), earlier, preferred_element_type=F32
    ).reshape(2, n_experts, rows)
    totals = jnp.sum(marks[0].astype(F32), axis=1)
    offset = jnp.stack([jnp.zeros_like(totals), totals])
    places = jnp.sum(
        jnp.where(marks, before + offset[:, :, None], 0.0), axis=1
    ).astype(jnp.int32)
    group_of, inner = flat // local, flat % local
    base, size = jnp.zeros_like(inner), jnp.full_like(inner, sizes[0])
    base = jnp.where(inner >= sizes[0], sizes[0], base)
    size = jnp.where(inner >= sizes[0], local - sizes[0], size)
    ranked = base * groups + group_of * size + inner - base
    kept = (flat >= 0) & (places < capacity)
    slots = jnp.where(kept, ranked * room + places, -1)
    token_ids = jnp.broadcast_to(adapter_ids[:, None], (n_images, padded)).reshape(1, rows)
    slot_columns = slots.reshape(2, n_images, padded).transpose(1, 2, 0)
    side = jnp.concatenate([slots, token_ids], axis=0)
    side_all = gather_blocks(side, "expert")
    upstream_all = gather_blocks(upstream.reshape(rows, width), "expert")

    gain_one = ln_gain1.astype(F32).reshape(1, width)
    gain_two = ln_gain2.astype(F32).reshape(1, width)
    router_t = router_weight.T
    qkv_a_t = qkv_a.transpose(0, 2, 1)
    out_a_t = out_a.transpose(0, 2, 1)
    router_a_t = router_a.transpose(0, 2, 1)
    shared = (gain_one, gain_two, qkv_weight, out_weight, router_t)
    adapters = (qkv_a_t, qkv_b, out_a_t, out_b, router_a_t, router_b)
    grid_of = functools.partial(pltpu.PrefetchScalarGridSpec, num_scalar_prefetch=1)
    forward_out = (
        jax.ShapeDtypeStruct((n_images, padded, 3 * width), LOW),
        jax.ShapeDtypeStruct((n_images, padded, width), LOW),
        jax.ShapeDtypeStruct((n_images, padded, width), F32),
        jax.ShapeDtypeStruct((n_images, padded, width), LOW),
        jax.ShapeDtypeStruct((n_images, padded, 2), F32),
        jax.ShapeDtypeStruct((n_images, 2, padded), F32),
    )
    qkv, context, hidden, normed, gates, gate_rows = pl.pallas_call(
        functools.partial(forward_kernel, seq_len),
        out_shape=forward_out,
        grid_spec=grid_of(
            grid=(n_images,),
            in_specs=[per_image(a) for a in (images, picks, pick_rows)]
            + [whole(a) for a in shared]
            + [per_adapter(a) for a in adapters],
            out_specs=[per_image(a) for a in forward_out],
        ),
        name="attend",
        cost_estimate=work_of(20),
    )(adapter_ids, images, picks, pick_rows, *shared, *adapters)

    normed_all = gather_blocks(normed.reshape(rows, width), "expert")
    sources = block_sources("expert")
    gates_all = gather_blocks(gate_rows.transpose(1, 0, 2).reshape(2, rows), "expert")
    up_a_t = up_a.transpose(0, 1, 3, 2).reshape(local, low_cols, width)
    up_b_flat = up_b.reshape(local, low_cols, ff_width)
    down_a_t = down_a.transpose(0, 1, 3, 2).reshape(local, low_cols, ff_width)
    down_b_flat = down_b.reshape(local, low_cols, width)
    cols = 2 * width + 2 * ff_width
    backs, sums, raw = [], [], []
    for piece, (at, here) in enumerate(zip(starts, sizes)):

        def of_expert(array, at=at):
            rank = len(array.shape)
            return pl.BlockSpec(
                (1,) + array.shape[1:], lambda i, s: (i + at,) + (0,) * (rank - 1)
            )

        weights = (up_weight, down_weight, up_a_t, up_b_flat, down_a_t, down_b_flat)
        lowest, together = (0, sizes[0]) if piece == 0 else (sizes[0], local - sizes[0])
        first = lowest * groups + lax.axis_index("expert") * together + at - lowest
        first = first.astype(jnp.int32)
        gathered = (*side_all, *gates_all, *normed_all, *upstream_all)
        after = tuple(raw[-1:])
        n_rows = groups * room
        back, grads = pl.pallas_call(
            functools.partial(expert_kernel, len(after), groups),
            out_shape=(
                jax.ShapeDtypeStruct((groups, here, room, 2 * width), LOW),
                jax.ShapeDtypeStruct((here, low_cols, cols), LOW),
            ),
            grid_spec=grid_of(
                grid=(here,),
                in_specs=[whole(a) for a in gathered]
                + [of_expert(a) for a in weights]
                + [pl.BlockSpec(memory_space=pl.ANY) for a in after],
                out_specs=[
                    pl.BlockSpec((groups, 1, room, 2 * width), lambda i, s: (0, i, 0, 0)),
                    pl.BlockSpec((1, low_cols, cols), lambda i, s: (i, 0, 0)),
                ],
                scratch_shapes=[
                    pltpu.VMEM((n_rows, width), LOW),
                    pltpu.VMEM((n_rows, width), LOW),
                    pltpu.VMEM((n_rows, low_cols), F32),
                    pltpu.VMEM((n_rows, width), F32),
                    pltpu.VMEM((n_rows, width), F32),
                    pltpu.VMEM((n_rows, low_cols), F32),
                    pltpu.VMEM((n_rows, low_cols), F32),
                    pltpu.VMEM((2, low_cols, n_rows), LOW),
                ],
            ),
            cost_estimate=work_of(14 * here),
        )(jnp.concatenate([first.reshape(1), sources]), *gathered, *weights, *after)
        raw.append(back)
        if piece != 1:
            back = back if piece == 0 else jnp.concatenate(raw[1:], axis=1)
            back = lax.all_to_all(back, "expert", split_axis=0, concat_axis=0, tiled=True)
            backs.append(back)
        sums.append(grads)
        if piece == 1:
            sums = list(lax.psum(tuple(sums), "dp"))
        if piece == 2:
            sums[2] = direct_parts(grads, "dp")
    backs = [back.reshape(-1, 2 * width) for back in backs]

    grad_cols = 8 * width
    tiles = grad_cols // 128
    out_types = (
        jax.ShapeDtypeStruct((n_images, seq_len, width), LOW),
        jax.ShapeDtypeStruct((n_images, seq_len, width), F32),
        jax.ShapeDtypeStruct((n_adapt, tiles, rank, 128), LOW),
    )
    by_image = (images, upstream, hidden, normed, qkv, context, gates, picks, slot_columns)
    block_out, input_grad, own_grads = pl.pallas_call(
        functools.partial(backward_kernel, seq_len),
        out_shape=out_types,
        grid_spec=grid_of(
            grid=(n_images,),
            in_specs=[per_image(a) for a in by_image]
            + [whole(a) for a in shared]
            + [per_adapter(a) for a in adapters]
            + [whole(a) for a in backs],
            out_specs=[per_image(out_types[0]), per_image(out_types[1]), whole(out_types[2])],
            scratch_shapes=[
                pltpu.VMEM((n_adapt, rank, grad_cols), F32),
                pltpu.VMEM((padded, 3 * width), LOW),
            ],
        ),
        name="attend_back",
        cost_estimate=work_of(40),
    )(adapter_ids, *by_image, *shared, *adapters, *backs)
    last = direct_gather(sum_after(sums[2], own_grads), "dp")
    sums[2] = last.reshape((sizes[2],) + sums[0].shape[1:])
    part = exchange_sum(own_grads.reshape(-1, 128), "expert")
    part = exchange_sum(part, "dp")
    part = exchange_gather(part, "dp")
    part = exchange_gather(part, "expert")
    own_grads = part.reshape(n_adapt, tiles, rank, 128)

    def own_part(start, length):
        part = own_grads[:, start // 128 : -(-(start + length) // 128)].astype(F32)
        return part.transpose(0, 2, 1, 3).reshape(n_adapt, rank, -1)[:, :, :length]

    grad_qkv_a = own_part(0, width).transpose(0, 2, 1)
    grad_qkv_b = own_part(width, 3 * width)
    grad_out_a = own_part(4 * width, width).transpose(0, 2, 1)
    grad_out_b = own_part(5 * width, width)
    grad_router_a = own_part(6 * width, width).transpose(0, 2, 1)
    grad_router_b = own_part(7 * width, n_experts)

    def expert_part(start, length):
        parts = [total[:, :, start : start + length].astype(F32) for total in sums]
        return jnp.concatenate(parts, axis=0).reshape(local, n_adapt, rank, length)

    grad_up_a = expert_part(0, width).transpose(0, 1, 3, 2)
    grad_up_b = expert_part(width, ff_width)
    grad_down_a = expert_part(width + ff_width, ff_width).transpose(0, 1, 3, 2)
    grad_down_b = expert_part(width + 2 * ff_width, width)
    return (
        block_out,
        input_grad,
        grad_qkv_a,
        grad_qkv_b,
        grad_out_a,
        grad_out_b,
        grad_router_a,
        grad_router_b,
        grad_up_a,
        grad_up_b,
        grad_down_a,
        grad_down_b,
    )


def solution(mesh):
    tokens = P(("dp", "expert"), None, None)
    experts = P("expert", None, None, None)
    weights = P("expert", None, None)
    placed = (
        (tokens, P(("dp", "expert")), tokens, tokens)
        + (P(),) * 5
        + (weights,) * 2
        + (P(),) * 6
        + (experts,) * 4
    )

    return jax.shard_map(
        body,
        mesh=mesh,
        in_specs=placed,
        out_specs=(tokens, tokens) + (P(),) * 6 + (experts,) * 4,
        check_vma=False,
    )
```
